16 devices in a mesh: batch: 4 (over z, y), seq: 4 (over x, core).
Axes of the slice: x: 2, y: 2, z: 2, core: 2. Of those that a mesh axis runs over, the one named last changes fastest.
Arguments:
- hidden: bfloat16 [128, 2048], P('batch'), parts along dimension 0
- lengths: int32 [128], P('batch'), parts along dimension 0
- c_kv: bfloat16 [128, 4096, 512], P('batch', 'seq'), parts along dimension 0
- k_rope: bfloat16 [128, 4096, 64], P('batch', 'seq'), parts along dimension 0
- w_uq: bfloat16 [2048, 16, 128], P(None, 'seq')
- w_qr: bfloat16 [2048, 16, 64], P(None, 'seq')
- w_uk: bfloat16 [16, 128, 512], P('seq')
- w_uv: bfloat16 [16, 512, 128], P('seq')
- w_o: bfloat16 [16, 128, 2048], P('seq')
Outputs:
- output: bfloat16 [128, 2048], P('batch'), parts along dimension 0
There are 4 independent parts. The reference program is written for one: setup_inputs(seed, part) draws one part's arguments, and reference() takes and returns one part's arrays. A program takes and returns all parts, laid end to end along the dimension named above; an argument that names none is the same for every part.
All inputs are finite; a program needn't handle non-finite values.
Results may differ from the reference program's by a relative error of at most 0.00323331.
Values are sent between devices in bfloat16 or wider.
A program may use at most 1 GiB of HBM per device.

```python
import math
import jax
import jax.numpy as jnp
from jax import lax

BATCH_ROWS = 32
D_MODEL = 2048
NUM_HEADS = 16
SHARD_LEN = 1024
CACHE_LEN = 4096
LATENT_DIM = 512
ROPE_DIM = 64
NOPE_DIM = 128
VALUE_DIM = 128
SCORE_SCALE = 1.0 / math.sqrt(NOPE_DIM + ROPE_DIM)
SCORE_GAIN = 0.75 * math.sqrt(math.log(CACHE_LEN))


def draw_lengths(len_key):
    perm_key, long_key, short_key = jax.random.split(len_key, 3)
    row_rank = jax.random.permutation(perm_key, BATCH_ROWS)
    long_len = jax.random.randint(long_key, (BATCH_ROWS,), CACHE_LEN - SHARD_LEN + 1, CACHE_LEN + 1)
    long_len = jnp.where(row_rank == 0, CACHE_LEN, long_len)
    short_len = jax.random.randint(short_key, (BATCH_ROWS,), 1, CACHE_LEN // 4 + 1)
    return jnp.where(row_rank < max(1, BATCH_ROWS // 4), long_len, short_len).astype(jnp.int32)


def setup_inputs(seed: int = 0, part: int = 0) -> dict:
    part_key = jax.random.fold_in(jax.random.key(seed), part)
    key_list = jax.random.split(part_key, 4)
    weight_keys = jax.random.split(jax.random.key(seed + 1), 5)
    hidden = jax.random.normal(key_list[0], (BATCH_ROWS, D_MODEL), jnp.float32)
    c_kv = jax.random.normal(key_list[2], (BATCH_ROWS, CACHE_LEN, LATENT_DIM), jnp.float32)
    k_rope = jax.random.normal(key_list[3], (BATCH_ROWS, CACHE_LEN, ROPE_DIM), jnp.float32)
    w_uq = jax.random.normal(weight_keys[0], (D_MODEL, NUM_HEADS, NOPE_DIM), jnp.float32) * D_MODEL ** -0.5
    w_qr = jax.random.normal(weight_keys[1], (D_MODEL, NUM_HEADS, ROPE_DIM), jnp.float32) * D_MODEL ** -0.5
    w_uk = jax.random.normal(weight_keys[2], (NUM_HEADS, NOPE_DIM, LATENT_DIM), jnp.float32) * (SCORE_GAIN * NOPE_DIM ** -0.5)
    w_uv = jax.random.normal(weight_keys[3], (NUM_HEADS, LATENT_DIM, VALUE_DIM), jnp.float32) * LATENT_DIM ** -0.5
    w_o = jax.random.normal(weight_keys[4], (NUM_HEADS, VALUE_DIM, D_MODEL), jnp.float32) * (NUM_HEADS * VALUE_DIM) ** -0.5
    return dict(hidden=hidden.astype(jnp.bfloat16), lengths=draw_lengths(key_list[1]), c_kv=c_kv.astype(jnp.bfloat16), k_rope=k_rope.astype(jnp.bfloat16), w_uq=w_uq.astype(jnp.bfloat16), w_qr=w_qr.astype(jnp.bfloat16), w_uk=w_uk.astype(jnp.bfloat16), w_uv=w_uv.astype(jnp.bfloat16), w_o=w_o.astype(jnp.bfloat16))


def reference(hidden, lengths, c_kv, k_rope, w_uq, w_qr, w_uk, w_uv, w_o):
    hidden_f32 = hidden.astype(jnp.float32)
    q_nope = jnp.einsum('bd,dhk->bhk', hidden_f32, w_uq.astype(jnp.float32)).astype(jnp.bfloat16)
    q_rope = jnp.einsum('bd,dhr->bhr', hidden_f32, w_qr.astype(jnp.float32)).astype(jnp.bfloat16)
    q_lat = jnp.einsum('bhk,hkc->bhc', q_nope.astype(jnp.float32), w_uk.astype(jnp.float32)).astype(jnp.bfloat16)
    positions = jnp.arange(CACHE_LEN)

    def one_row(row_args):
        q_lat_row, q_rope_row, c_row, k_row, row_len = row_args
        scores = (jnp.dot(q_lat_row, c_row.T, preferred_element_type=jnp.float32) + jnp.dot(q_rope_row, k_row.T, preferred_element_type=jnp.float32)) * SCORE_SCALE
        scores = jnp.where(positions[None, :] < row_len, scores, -jnp.inf)
        row_max = jnp.max(scores, axis=1, keepdims=True)
        p_weights = jnp.exp(scores - row_max)
        weight_sum = jnp.sum(p_weights, axis=1, keepdims=True)
        latent_sum = jnp.dot(p_weights.astype(jnp.bfloat16), c_row, preferred_element_type=jnp.float32)
        return (latent_sum / weight_sum).astype(jnp.bfloat16)

    o_lat = lax.map(one_row, (q_lat, q_rope, c_kv, k_rope, lengths))
    o_val = jnp.einsum('bhc,hcv->bhv', o_lat.astype(jnp.float32), w_uv.astype(jnp.float32)).astype(jnp.bfloat16)
    y_sum = jnp.einsum('bhv,hvd->bd', o_val.astype(jnp.float32), w_o.astype(jnp.float32))
    return (hidden_f32 + y_sum).astype(jnp.bfloat16)
```

```python
import math

import jax
import jax.numpy as jnp
from jax import lax
from jax.experimental import pallas as pl
from jax.experimental.pallas import tpu as pltpu
from jax.sharding import PartitionSpec as P

MESH = pl.DeviceIdType.MESH
F32 = jnp.float32
BF16 = jnp.bfloat16
GROUP = 4
STAT = 128


def dot(a, b):
    return jnp.dot(a, b, preferred_element_type=F32)


def dot_t(a, b):
    return lax.dot_general(a, b, (((1,), (1,)), ((), ())), preferred_element_type=F32)


def iota(shape, dim):
    return lax.broadcasted_iota(jnp.int32, shape, dim)


def kernel(
    len_hbm, hid_hbm, hid3_hbm, wuq_hbm, wqr_hbm, wuk_hbm, wuv_hbm, wo_hbm, ckv_hbm, kr_hbm,
    out_ref,
    len_s, hid_v, hid3_v, wuq_v, wqr_v, wuk_v, wuv_v, wo_v, ckv_v, kr_v,
    em_v, qall, sbuf, acc_src, r1, s2, keep_v, r2, y_src, yr1, yc, yr2, f_src, f_rcv,
    w_sem, ckv_sem, kr_sem, q_send, q_recv, a_send, a_recv, c_send, c_recv, y_send, y_recv,
):
    n_rows = ckv_hbm.shape[0]
    shard = ckv_hbm.shape[1]
    lat = ckv_hbm.shape[2]
    rope = kr_hbm.shape[1]
    nope = wuq_hbm.shape[1]
    n_pair = n_rows // 2
    n_group = n_pair // GROUP
    d_model = hid_hbm.shape[1]
    half_d = d_model // 2
    scale = 1.0 / math.sqrt(nope + rope)

    me = lax.axis_index("seq")
    x = lax.div(me, 2)
    c = lax.rem(me, 2)
    sib = 2 * x + (1 - c)
    cnt = 2 * (1 - x) + c

    def load(src, dst, sem):
        return pltpu.make_async_copy(src, dst, sem)

    weights = [
        load(hid_hbm, hid_v, w_sem.at[0]),
        load(wuq_hbm, wuq_v, w_sem.at[1]),
        load(wqr_hbm, wqr_v, w_sem.at[2]),
        load(wuk_hbm, wuk_v, w_sem.at[3]),
        load(len_hbm, len_s, w_sem.at[4]),
        load(hid3_hbm, hid3_v, w_sem.at[5]),
    ]
    late_weights = [
        load(wuv_hbm, wuv_v, w_sem.at[6]),
        load(wo_hbm, wo_v, w_sem.at[7]),
    ]

    def ckv_load(b):
        return load(ckv_hbm.at[b], ckv_v.at[b], ckv_sem.at[b])

    def kr_load(b):
        return load(kr_hbm.at[b], kr_v.at[b], kr_sem.at[b])

    for w in weights:
        w.start()

    barrier = pltpu.get_barrier_semaphore()
    for peer in (sib, cnt):
        pl.semaphore_signal(barrier, inc=1, device_id={"seq": peer}, device_id_type=MESH)

    def start_rows(b, carry):
        kr_load(b).start()
        ckv_load(b).start()
        return carry

    lax.fori_loop(0, n_rows // 2, start_rows, 0)
    for w in late_weights:
        w.start()
    lax.fori_loop(n_rows // 2, n_rows, start_rows, 0)

    def remote(src, dst, send, recv, peer):
        return pltpu.make_async_remote_copy(
            src_ref=src, dst_ref=dst, send_sem=send, recv_sem=recv,
            device_id={"seq": peer}, device_id_type=MESH,
        )

    n_head = wqr_hbm.shape[0] // rope
    n_local = n_rows * n_head
    lane_h = iota((n_rows, 4 * nope), 1) % n_head
    spread = (iota((nope, n_head * nope), 1) // n_head == iota((nope, n_head * nope), 0)).astype(F32).astype(BF16)
    for i in (0, 1):
        weights[i].wait()
    for k in range(d_model // nope):
        wide = dot(hid_v[:, k * nope:(k + 1) * nope], spread)
        for h in range(n_head):
            em_v[h * n_rows:(h + 1) * n_rows, k * n_head * nope:(k + 1) * n_head * nope] = jnp.where(
                lane_h == h, wide, 0.0).astype(BF16)
    q_n = dot(em_v[...], wuq_v[...]).astype(BF16)
    for i in (2, 3, 4, 5):
        weights[i].wait()
    q_r = dot_t(hid_v[...], wqr_v[...]).astype(BF16)

    def row_of(r):
        j = (r // 4) % 2
        return 2 * (r // 8) + j + x - 2 * j * x

    r_id = iota((n_local, n_local), 0)
    col = iota((n_local, n_local), 1)
    perm = (col == (r_id % 4) * n_rows + row_of(r_id)).astype(F32).astype(BF16)
    q_p = dot(perm, q_n)
    r_h = iota((n_local, nope), 0) % 4
    q_wide = jnp.concatenate([jnp.where(r_h == h, q_p, 0.0).astype(BF16) for h in range(n_head)], axis=1)
    q_l = dot(q_wide, wuk_v[...]).astype(BF16)
    r_id = iota((n_local, n_rows), 0)
    rep = (iota((n_local, n_rows), 1) == row_of(r_id)).astype(F32).astype(BF16)
    q_r = dot(rep, q_r)
    q_r = jnp.where(iota((n_local, n_head * rope), 1) // rope == iota((n_local, n_head * rope), 0) % 4, q_r, 0.0)
    fold = (iota((n_head * rope, STAT), 0) % rope == iota((n_head * rope, STAT), 1)).astype(F32).astype(BF16)
    q_r = dot(q_r.astype(BF16), fold).astype(BF16)
    for p in range(n_pair):
        qall[me, p, :, 0:lat] = q_l[8 * p:8 * p + 8]
        qall[me, p, :, lat:lat + STAT] = q_r[8 * p:8 * p + 8]

    pl.semaphore_wait(barrier, 2)

    def q_copy(kind, g):
        slot, peer = ((me, sib), (me, cnt), (cnt, sib))[kind]
        part = qall.at[slot, pl.ds(GROUP * g, GROUP)]
        return remote(part, part, q_send.at[kind, g], q_recv.at[kind, g], peer)

    for g in range(n_group):
        q_copy(1, g).start()
    for g in range(n_group):
        q_copy(0, g).start()

    upper8 = iota((8, lat + STAT), 0) < 4

    def scores(p):
        tiles = [qall[s, p].astype(F32) for s in range(4)]
        q_even = jnp.concatenate([jnp.where(upper8, tiles[0], tiles[2]), jnp.where(upper8, tiles[1], tiles[3])], axis=0)
        q_odd = jnp.concatenate([jnp.where(upper8, tiles[2], tiles[0]), jnp.where(upper8, tiles[3], tiles[1])], axis=0)
        for i, q in enumerate((q_even, q_odd)):
            q = q.astype(BF16)
            b = 2 * p + i
            s = dot_t(q[:, :lat], ckv_v[b]) + dot(q[:, lat:lat + rope], kr_v[b])
            sbuf[p % 2, i] = s

    def wait_rows(p):
        for i in (0, 1):
            kr_load(2 * p + i).wait()
            ckv_load(2 * p + i).wait()

    stat_lane = iota((16, STAT), 1) < STAT // 2

    def attend(p):
        for i in (0, 1):
            b = 2 * p + i
            s = sbuf[p % 2, i] * scale
            pos = me * shard + iota(s.shape, 1)
            s = jnp.where(pos < len_s[b], s, -jnp.inf)
            m = jnp.max(s, axis=1, keepdims=True)
            e = jnp.exp(s - jnp.where(m > -jnp.inf, m, 0.0))
            l = jnp.sum(e, axis=1, keepdims=True)
            acc = dot(e.astype(BF16), ckv_v[b])
            stat = jnp.where(stat_lane, m, l)
            for k in (0, 1):
                acc_src[k, b, :, 0:lat] = acc[8 * k:8 * k + 8]
                acc_src[k, b, :, lat:lat + STAT] = stat[8 * k:8 * k + 8]

    def pair_copy(p):
        rows = pl.ds(2 * p, 2)
        return remote(acc_src.at[1 - c, rows], r1.at[rows], a_send.at[p], a_recv.at[p], sib)

    def chip_copy(p):
        return remote(s2.at[p], r2.at[p], c_send.at[p], c_recv.at[p], cnt)

    def merge(a, b):
        m1, l1 = a[:, lat:lat + 1], a[:, lat + STAT // 2:lat + STAT // 2 + 1]
        m2, l2 = b[:, lat:lat + 1], b[:, lat + STAT // 2:lat + STAT // 2 + 1]
        m = jnp.maximum(m1, m2)
        shift = jnp.where(m > -jnp.inf, m, 0.0)
        w1, w2 = jnp.exp(m1 - shift), jnp.exp(m2 - shift)
        return w1 * a[:, :lat] + w2 * b[:, :lat], m, w1 * l1 + w2 * l2

    stat_lane8 = iota((8, STAT), 1) < STAT // 2

    def merge_pair(p):
        pair_copy(p).wait_recv()
        both = []
        for i in (0, 1):
            acc, m, l = merge(acc_src[c, 2 * p + i], r1[2 * p + i])
            both.append((acc, jnp.where(stat_lane8, m, l)))
        for k, (lo, hi) in enumerate(((0, lat), (lat, lat + STAT))):
            upper = upper8[:, lo:hi]
            zero = jnp.where(upper, both[0][k], both[1][k])
            one = jnp.where(upper, both[1][k], both[0][k])
            keep_v[p, :, lo:hi] = jnp.where(x == 0, zero, one)
            s2[p, :, lo:hi] = jnp.where(x == 0, one, zero)
        chip_copy(p).start()

    def o_rows(p):
        chip_copy(p).wait_recv()
        acc, _, l = merge(keep_v[p], r2[p])
        return acc / l

    n_out = 8 * GROUP

    def project(g):
        o_lat = jnp.concatenate([o_rows(GROUP * g + i) for i in range(GROUP)], axis=0).astype(BF16)
        head = iota((n_out, nope), 0) % 4
        wide = jnp.concatenate(
            [jnp.where(head == h, dot(o_lat, wuv_v[h]), 0.0).astype(BF16) for h in range(n_head)], axis=1)
        r = iota((8, n_out), 1)
        gather = (iota((8, n_out), 0) == row_of(r)).astype(F32).astype(BF16)
        o_val = dot(gather, wide).astype(BF16)
        for k in (0, 1):
            y_src[g, k] = dot(o_val, wo_v[:, k * half_d:(k + 1) * half_d])

    def y_copy(kind, g):
        if kind == 0:
            src, dst, peer = y_src.at[g, 1 - c], yr1.at[g], sib
        elif kind == 1:
            src, dst, peer = yc.at[g], yr2.at[g], cnt
        else:
            src, dst, peer = f_src.at[g], f_rcv.at[g], sib
        return remote(src, dst, y_send.at[kind, g], y_recv.at[kind, g], peer)

    def y_chip(g):
        y_copy(0, g).wait_recv()
        yc[g] = y_src[g, c] + yr1[g]
        y_copy(1, g).start()

    def y_final(g):
        y_copy(1, g).wait_recv()
        hid = hid3_v[c, g].astype(F32)
        f_src[g] = (hid + (yc[g] + yr2[g])).astype(BF16)
        y_copy(2, g).start()

    def store(g):
        y_copy(2, g).wait_recv()
        mine, other = f_src[g].astype(F32), f_rcv[g].astype(F32)
        out_ref[g, :, 0:half_d] = jnp.where(c == 0, mine, other).astype(BF16)
        out_ref[g, :, half_d:d_model] = jnp.where(c == 0, other, mine).astype(BF16)

    def step(j, carry, with_merge):
        wait_rows(j)
        scores(j)
        attend(j - 1)
        pair_copy(j - 1).start()
        if with_merge:
            merge_pair(j - GROUP)
        return carry

    for g in range(n_group):
        q_copy(1, g).wait_recv()
        q_copy(2, g).start()
        q_copy(0, g).wait_recv()
        q_copy(2, g).wait_recv()
        if g == 0:
            wait_rows(0)
            scores(0)
        lax.fori_loop(max(1, GROUP * g), GROUP * (g + 1), lambda j, cy, m=g > 0: step(j, cy, m), 0)
        if g == 2:
            for w in late_weights:
                w.wait()
        if g >= 2:
            project(g - 2)
            y_copy(0, g - 2).start()
        if g >= 3:
            y_chip(g - 3)
    attend(n_pair - 1)
    pair_copy(n_pair - 1).start()
    for p in range(n_pair - GROUP, n_pair - 1):
        merge_pair(p)
    for g in range(n_group - 2, n_group):
        if g == n_group - 1:
            merge_pair(n_pair - 1)
            y_chip(n_group - 3)
            y_chip(n_group - 2)
            y_final(n_group - 4)
        project(g)
        y_copy(0, g).start()
    y_final(n_group - 3)
    y_final(n_group - 2)
    y_chip(n_group - 1)
    y_final(n_group - 1)
    for g in range(n_group):
        store(g)

    for g in range(n_group):
        for kind in range(3):
            q_copy(kind, g).wait_send()
            y_copy(kind, g).wait_send()

    def drain(p, carry):
        pair_copy(p).wait_send()
        chip_copy(p).wait_send()
        return carry

    lax.fori_loop(0, n_pair, drain, 0)


def solution(mesh):
    row_spec = P('batch', None)
    cache_spec = P('batch', 'seq', None)
    in_specs = (row_spec, P('batch'), cache_spec, cache_spec, P(None, 'seq', None), P(None, 'seq', None), P('seq', None, None), P('seq', None, None), P('seq', None, None))

    def mla_step(hidden, lengths, c_kv, k_rope, w_uq, w_qr, w_uk, w_uv, w_o):
        n_rows, d_model = hidden.shape
        _, shard, lat = c_kv.shape
        rope = k_rope.shape[2]
        n_head, nope = w_uq.shape[1], w_uq.shape[2]
        n_pair = n_rows // 2
        n_group = n_pair // GROUP
        wide = lat + STAT
        half = d_model // 2
        hid3 = jnp.transpose(hidden.reshape(n_group, 8, 2, half), (2, 0, 1, 3))
        operands = (
            lengths,
            hidden,
            hid3,
            w_uq.reshape(d_model * n_head, nope),
            jnp.transpose(w_qr, (1, 2, 0)).reshape(n_head * rope, d_model),
            w_uk.reshape(n_head * nope, lat),
            w_uv,
            w_o.reshape(n_head * w_o.shape[1], d_model),
            c_kv,
            jnp.transpose(k_rope, (0, 2, 1)),
        )
        vm = pltpu.VMEM
        dma = pltpu.SemaphoreType.DMA
        out = pl.pallas_call(
            kernel,
            out_shape=jax.ShapeDtypeStruct((n_group, 8, d_model), BF16),
            in_specs=[pl.BlockSpec(memory_space=pltpu.HBM)] * len(operands),
            out_specs=pl.BlockSpec(memory_space=pltpu.VMEM),
            scratch_shapes=[
                pltpu.SMEM((n_rows,), jnp.int32),
                vm(hidden.shape, BF16),
                vm(hid3.shape, BF16),
                vm(operands[3].shape, BF16),
                vm(operands[4].shape, BF16),
                vm(operands[5].shape, BF16),
                vm(operands[6].shape, BF16),
                vm(operands[7].shape, BF16),
                vm(c_kv.shape, BF16),
                vm(operands[9].shape, BF16),
                vm((n_head * n_rows, n_head * d_model), BF16),
                vm((4, n_pair, 8, wide), BF16),
                vm((2, 2, 16, shard), F32),
                vm((2, n_rows, 8, wide), F32),
                vm((n_rows, 8, wide), F32),
                vm((n_pair, 8, wide), F32),
                vm((n_pair, 8, wide), F32),
                vm((n_pair, 8, wide), F32),
                vm((n_group, 2, 8, half), F32),
                vm((n_group, 8, half), F32),
                vm((n_group, 8, half), F32),
                vm((n_group, 8, half), F32),
                vm((n_group, 8, half), BF16),
                vm((n_group, 8, half), BF16),
                dma((8,)),
                dma((n_rows,)),
                dma((n_rows,)),
                dma((3, n_group)),
                dma((3, n_group)),
                dma((n_pair,)),
                dma((n_pair,)),
                dma((n_pair,)),
                dma((n_pair,)),
                dma((3, n_group)),
                dma((3, n_group)),
            ],
            compiler_params=pltpu.CompilerParams(
                collective_id=0, has_side_effects=True, vmem_limit_bytes=62 * 1024 * 1024,
            ),
            name="mla_decode",
        )(*operands)
        return out.reshape(n_rows, d_model)

    return jax.shard_map(mla_step, mesh=mesh, in_specs=in_specs, out_specs=row_spec, check_vma=False)
```

```python
import math

import jax
import jax.numpy as jnp
from jax import lax
from jax.experimental import pallas as pl
from jax.experimental.pallas import tpu as pltpu
from jax.sharding import PartitionSpec as P

MESH = pl.DeviceIdType.MESH
F32 = jnp.float32
BF16 = jnp.bfloat16
GROUP = 4
STAT = 128


def dot(a, b):
    return jnp.dot(a, b, preferred_element_type=F32)


def dot_t(a, b):
    return lax.dot_general(a, b, (((1,), (1,)), ((), ())), preferred_element_type=F32)


def iota(shape, dim):
    return lax.broadcasted_iota(jnp.int32, shape, dim)


def kernel(
    len_hbm, hid_hbm, hid3_hbm, wuq_hbm, wqr_hbm, wuk_hbm, wuv_hbm, wo_hbm, ckv_hbm, kr_hbm,
    out_ref,
    len_s, hid_v, hid3_v, wuq_v, wqr_v, wuk_v, wuv_v, wo_v, ckv_v, kr_v,
    em_v, qall, sbuf, acc_src, r1, s2, keep_v, r2, y_src, yr1, yc, yr2, f_src, f_rcv,
    w_sem, ckv_sem, kr_sem, q_send, q_recv, a_send, a_recv, c_send, c_recv, y_send, y_recv,
):
    n_rows = ckv_hbm.shape[0]
    shard = ckv_hbm.shape[1]
    lat = ckv_hbm.shape[2]
    rope = kr_hbm.shape[1]
    nope = wuq_hbm.shape[1]
    n_pair = n_rows // 2
    n_group = n_pair // GROUP
    d_model = hid_hbm.shape[1]
    half_d = d_model // 2
    scale = 1.0 / math.sqrt(nope + rope)

    me = lax.axis_index("seq")
    x = lax.div(me, 2)
    c = lax.rem(me, 2)
    sib = 2 * x + (1 - c)
    cnt = 2 * (1 - x) + c

    def load(src, dst, sem):
        return pltpu.make_async_copy(src, dst, sem)

    weights = [
        load(hid_hbm, hid_v, w_sem.at[0]),
        load(wuq_hbm, wuq_v, w_sem.at[1]),
        load(wqr_hbm, wqr_v, w_sem.at[2]),
        load(wuk_hbm, wuk_v, w_sem.at[3]),
        load(len_hbm, len_s, w_sem.at[4]),
        load(hid3_hbm, hid3_v, w_sem.at[5]),
    ]
    late_weights = [
        load(wuv_hbm, wuv_v, w_sem.at[6]),
        load(wo_hbm, wo_v, w_sem.at[7]),
    ]

    def ckv_load(b):
        return load(ckv_hbm.at[b], ckv_v.at[b], ckv_sem.at[b])

    def kr_load(b):
        return load(kr_hbm.at[b], kr_v.at[b], kr_sem.at[b])

    for w in weights:
        w.start()

    barrier = pltpu.get_barrier_semaphore()
    for peer in (sib, cnt):
        pl.semaphore_signal(barrier, inc=1, device_id={"seq": peer}, device_id_type=MESH)

    def start_rows(b, carry):
        kr_load(b).start()
        ckv_load(b).start()
        return carry

    lax.fori_loop(0, n_rows // 2, start_rows, 0)
    for w in late_weights:
        w.start()
    lax.fori_loop(n_rows // 2, n_rows, start_rows, 0)

    def remote(src, dst, send, recv, peer):
        return pltpu.make_async_remote_copy(
            src_ref=src, dst_ref=dst, send_sem=send, recv_sem=recv,
            device_id={"seq": peer}, device_id_type=MESH,
        )

    n_head = wqr_hbm.shape[0] // rope
    n_local = n_rows * n_head
    lane_h = iota((n_rows, 4 * nope), 1) % n_head
    spread = (iota((nope, n_head * nope), 1) // n_head == iota((nope, n_head * nope), 0)).astype(F32).astype(BF16)
    for i in (0, 1):
        weights[i].wait()
    for k in range(d_model // nope):
        wide = dot(hid_v[:, k * nope:(k + 1) * nope], spread)
        for h in range(n_head):
            em_v[h * n_rows:(h + 1) * n_rows, k * n_head * nope:(k + 1) * n_head * nope] = jnp.where(
                lane_h == h, wide, 0.0).astype(BF16)
    q_n = dot(em_v[...], wuq_v[...]).astype(BF16)
    for i in (2, 3, 4, 5):
        weights[i].wait()
    q_r = dot_t(hid_v[...], wqr_v[...]).astype(BF16)

    def row_of(r):
        j = (r // 4) % 2
        return 2 * (r // 8) + j + x - 2 * j * x

    r_id = iota((n_local, n_local), 0)
    col = iota((n_local, n_local), 1)
    perm = (col == (r_id % 4) * n_rows + row_of(r_id)).astype(F32).astype(BF16)
    q_p = dot(perm, q_n)
    r_h = iota((n_local, nope), 0) % 4
    q_wide = jnp.concatenate([jnp.where(r_h == h, q_p, 0.0).astype(BF16) for h in range(n_head)], axis=1)
    q_l = dot(q_wide, wuk_v[...]).astype(BF16)
    r_id = iota((n_local, n_rows), 0)
    rep = (iota((n_local, n_rows), 1) == row_of(r_id)).astype(F32).astype(BF16)
    q_r = dot(rep, q_r)
    q_r = jnp.where(iota((n_local, n_head * rope), 1) // rope == iota((n_local, n_head * rope), 0) % 4, q_r, 0.0)
    fold = (iota((n_head * rope, STAT), 0) % rope == iota((n_head * rope, STAT), 1)).astype(F32).astype(BF16)
    q_r = dot(q_r.astype(BF16), fold).astype(BF16)
    for p in range(n_pair):
        qall[me, p, :, 0:lat] = q_l[8 * p:8 * p + 8]
        qall[me, p, :, lat:lat + STAT] = q_r[8 * p:8 * p + 8]

    pl.semaphore_wait(barrier, 2)

    def q_copy(kind, g):
        slot, peer = ((me, sib), (me, cnt), (cnt, sib))[kind]
        part = qall.at[slot, pl.ds(GROUP * g, GROUP)]
        return remote(part, part, q_send.at[kind, g], q_recv.at[kind, g], peer)

    for g in range(n_group):
        q_copy(1, g).start()
    for g in range(n_group):
        q_copy(0, g).start()

    upper8 = iota((8, lat + STAT), 0) < 4

    def scores(p):
        tiles = [qall[s, p].astype(F32) for s in range(4)]
        q_even = jnp.concatenate([jnp.where(upper8, tiles[0], tiles[2]), jnp.where(upper8, tiles[1], tiles[3])], axis=0)
        q_odd = jnp.concatenate([jnp.where(upper8, tiles[2], tiles[0]), jnp.where(upper8, tiles[3], tiles[1])], axis=0)
        for i, q in enumerate((q_even, q_odd)):
            q = q.astype(BF16)
            b = 2 * p + i
            s = dot_t(q[:, :lat], ckv_v[b]) + dot(q[:, lat:lat + rope], kr_v[b])
            sbuf[p % 2, i] = s

    def wait_rows(p):
        for i in (0, 1):
            kr_load(2 * p + i).wait()
            ckv_load(2 * p + i).wait()

    stat_lane = iota((16, STAT), 1) < STAT // 2

    def attend(p):
        for i in (0, 1):
            b = 2 * p + i
            s = sbuf[p % 2, i] * scale
            pos = me * shard + iota(s.shape, 1)
            s = jnp.where(pos < len_s[b], s, -jnp.inf)
            m = jnp.max(s, axis=1, keepdims=True)
            e = jnp.exp(s - jnp.where(m > -jnp.inf, m, 0.0))
            l = jnp.sum(e, axis=1, keepdims=True)
            acc = dot(e.astype(BF16), ckv_v[b])
            stat = jnp.where(stat_lane, m, l)
            for k in (0, 1):
                acc_src[k, b, :, 0:lat] = acc[8 * k:8 * k + 8]
                acc_src[k, b, :, lat:lat + STAT] = stat[8 * k:8 * k + 8]

    def pair_copy(p):
        rows = pl.ds(2 * p, 2)
        return remote(acc_src.at[1 - c, rows], r1.at[rows], a_send.at[p], a_recv.at[p], sib)

    def chip_copy(p):
        return remote(s2.at[p], r2.at[p], c_send.at[p], c_recv.at[p], cnt)

    def merge(a, b):
        m1, l1 = a[:, lat:lat + 1], a[:, lat + STAT // 2:lat + STAT // 2 + 1]
        m2, l2 = b[:, lat:lat + 1], b[:, lat + STAT // 2:lat + STAT // 2 + 1]
        m = jnp.maximum(m1, m2)
        shift = jnp.where(m > -jnp.inf, m, 0.0)
        w1, w2 = jnp.exp(m1 - shift), jnp.exp(m2 - shift)
        return w1 * a[:, :lat] + w2 * b[:, :lat], m, w1 * l1 + w2 * l2

    stat_lane8 = iota((8, STAT), 1) < STAT // 2

    def merge_pair(p):
        both = []
        for i in (0, 1):
            acc, m, l = merge(acc_src[c, 2 * p + i], r1[2 * p + i])
            both.append((acc, jnp.where(stat_lane8, m, l)))
        for k, (lo, hi) in enumerate(((0, lat), (lat, lat + STAT))):
            upper = upper8[:, lo:hi]
            zero = jnp.where(upper, both[0][k], both[1][k])
            one = jnp.where(upper, both[1][k], both[0][k])
            keep_v[p, :, lo:hi] = jnp.where(x == 0, zero, one)
            s2[p, :, lo:hi] = jnp.where(x == 0, one, zero)

    def o_rows(p):
        acc, _, l = merge(keep_v[p], r2[p])
        return acc / l

    n_out = 8 * GROUP

    def project(g):
        o_lat = jnp.concatenate([o_rows(GROUP * g + i) for i in range(GROUP)], axis=0).astype(BF16)
        head = iota((n_out, nope), 0) % 4
        wide = jnp.concatenate(
            [jnp.where(head == h, dot(o_lat, wuv_v[h]), 0.0).astype(BF16) for h in range(n_head)], axis=1)
        r = iota((8, n_out), 1)
        gather = (iota((8, n_out), 0) == row_of(r)).astype(F32).astype(BF16)
        o_val = dot(gather, wide).astype(BF16)
        for k in (0, 1):
            y_src[g, k] = dot(o_val, wo_v[:, k * half_d:(k + 1) * half_d])

    def y_copy(kind, g):
        if kind == 0:
            src, dst, peer = y_src.at[g, 1 - c], yr1.at[g], sib
        elif kind == 1:
            src, dst, peer = yc.at[g], yr2.at[g], cnt
        else:
            src, dst, peer = f_src.at[g], f_rcv.at[g], sib
        return remote(src, dst, y_send.at[kind, g], y_recv.at[kind, g], peer)

    def y_chip(g):
        y_copy(0, g).wait_recv()
        yc[g] = y_src[g, c] + yr1[g]
        y_copy(1, g).start()

    def y_final(g):
        y_copy(1, g).wait_recv()
        hid = hid3_v[g, :, pl.ds(pl.multiple_of(c * half_d, half_d), half_d)].astype(F32)
        f_src[g] = (hid + (yc[g] + yr2[g])).astype(BF16)
        y_copy(2, g).start()

    def store(g):
        y_copy(2, g).wait_recv()
        mine, other = f_src[g].astype(F32), f_rcv[g].astype(F32)
        out_ref[g, :, 0:half_d] = jnp.where(c == 0, mine, other).astype(BF16)
        out_ref[g, :, half_d:d_model] = jnp.where(c == 0, other, mine).astype(BF16)

    def wait_group(g):
        for i in range(GROUP):
            chip_copy(GROUP * g + i).wait_recv()

    def step(j, with_merge, group=None):
        wait_rows(j)
        if with_merge:
            pair_copy(j - GROUP).wait_recv()
        if group is not None:
            wait_group(group)
        scores(j)
        attend(j - 1)
        if with_merge:
            merge_pair(j - GROUP)
        if group is not None:
            project(group)
        pair_copy(j - 1).start()
        if with_merge:
            chip_copy(j - GROUP).start()
        if group is not None:
            y_copy(0, group).start()

    def steps(lo, hi, with_merge):
        def body(j, carry):
            step(j, with_merge)
            return carry

        lax.fori_loop(lo, hi, body, 0)

    def forward(g):
        q_copy(1, g).wait_recv()
        q_copy(2, g).start()

    forward(0)
    for g in range(n_group):
        first, last = GROUP * g, GROUP * (g + 1)
        q_copy(0, g).wait_recv()
        q_copy(2, g).wait_recv()
        if g == 0:
            wait_rows(0)
            scores(0)
            first += 1
        if g == 2:
            for w in late_weights:
                w.wait()
        if g >= 2:
            step(first, True, g - 2)
            first += 1
        steps(first, GROUP * g + 2, g > 0)
        if g + 1 < n_group:
            forward(g + 1)
        if g >= 3:
            y_chip(g - 3)
        steps(GROUP * g + 2, last, g > 0)
    for p in range(n_pair - GROUP, n_pair - 1):
        pair_copy(p).wait_recv()
    wait_group(n_group - 2)
    attend(n_pair - 1)
    pair_copy(n_pair - 1).start()
    for p in range(n_pair - GROUP, n_pair - 1):
        merge_pair(p)
        chip_copy(p).start()
    y_chip(n_group - 3)
    y_final(n_group - 4)
    project(n_group - 2)
    y_copy(0, n_group - 2).start()
    pair_copy(n_pair - 1).wait_recv()
    merge_pair(n_pair - 1)
    chip_copy(n_pair - 1).start()
    y_chip(n_group - 2)
    y_final(n_group - 3)
    wait_group(n_group - 1)
    project(n_group - 1)
    y_copy(0, n_group - 1).start()
    y_final(n_group - 2)
    y_chip(n_group - 1)
    y_final(n_group - 1)
    for g in range(n_group):
        store(g)

    for g in range(n_group):
        for kind in range(3):
            q_copy(kind, g).wait_send()
            y_copy(kind, g).wait_send()

    def drain(p, carry):
        pair_copy(p).wait_send()
        chip_copy(p).wait_send()
        return carry

    lax.fori_loop(0, n_pair, drain, 0)


def solution(mesh):
    row_spec = P('batch', None)
    cache_spec = P('batch', 'seq', None)
    in_specs = (row_spec, P('batch'), cache_spec, cache_spec, P(None, 'seq', None), P(None, 'seq', None), P('seq', None, None), P('seq', None, None), P('seq', None, None))

    def mla_step(hidden, lengths, c_kv, k_rope, w_uq, w_qr, w_uk, w_uv, w_o):
        n_rows, d_model = hidden.shape
        _, shard, lat = c_kv.shape
        rope = k_rope.shape[2]
        n_head, nope = w_uq.shape[1], w_uq.shape[2]
        n_pair = n_rows // 2
        n_group = n_pair // GROUP
        wide = lat + STAT
        half = d_model // 2
        hid3 = hidden.reshape(n_group, 8, d_model)
        operands = (
            lengths,
            hidden,
            hid3,
            w_uq.reshape(d_model * n_head, nope),
            jnp.transpose(w_qr, (1, 2, 0)).reshape(n_head * rope, d_model),
            w_uk.reshape(n_head * nope, lat),
            w_uv,
            w_o.reshape(n_head * w_o.shape[1], d_model),
            c_kv,
            jnp.transpose(k_rope, (0, 2, 1)),
        )
        operands = tuple(pltpu.with_memory_space_constraint(a, pltpu.HBM) for a in operands)
        vm = pltpu.VMEM
        dma = pltpu.SemaphoreType.DMA
        out = pl.pallas_call(
            kernel,
            out_shape=jax.ShapeDtypeStruct((n_group, 8, d_model), BF16),
            in_specs=[pl.BlockSpec(memory_space=pltpu.HBM)] * len(operands),
            out_specs=pl.BlockSpec(memory_space=pltpu.VMEM),
            scratch_shapes=[
                pltpu.SMEM((n_rows,), jnp.int32),
                vm(hidden.shape, BF16),
                vm(hid3.shape, BF16),
                vm(operands[3].shape, BF16),
                vm(operands[4].shape, BF16),
                vm(operands[5].shape, BF16),
                vm(operands[6].shape, BF16),
                vm(operands[7].shape, BF16),
                vm(c_kv.shape, BF16),
                vm(operands[9].shape, BF16),
                vm((n_head * n_rows, n_head * d_model), BF16),
                vm((4, n_pair, 8, wide), BF16),
                vm((2, 2, 16, shard), F32),
                vm((2, n_rows, 8, wide), F32),
                vm((n_rows, 8, wide), F32),
                vm((n_pair, 8, wide), F32),
                vm((n_pair, 8, wide), F32),
                vm((n_pair, 8, wide), F32),
                vm((n_group, 2, 8, half), F32),
                vm((n_group, 8, half), F32),
                vm((n_group, 8, half), F32),
                vm((n_group, 8, half), F32),
                vm((n_group, 8, half), BF16),
                vm((n_group, 8, half), BF16),
                dma((8,)),
                dma((n_rows,)),
                dma((n_rows,)),
                dma((3, n_group)),
                dma((3, n_group)),
                dma((n_pair,)),
                dma((n_pair,)),
                dma((n_pair,)),
                dma((n_pair,)),
                dma((3, n_group)),
                dma((3, n_group)),
            ],
            compiler_params=pltpu.CompilerParams(
                collective_id=0, has_side_effects=True, vmem_limit_bytes=50 * 1024 * 1024,
            ),
            name="mla_decode",
        )(*operands)
        return out.reshape(n_rows, d_model)

    return jax.shard_map(mla_step, mesh=mesh, in_specs=in_specs, out_specs=row_spec, check_vma=False)
```

```python
import math

import jax
import jax.numpy as jnp
from jax import lax
from jax.experimental import pallas as pl
from jax.experimental.pallas import tpu as pltpu
from jax.sharding import PartitionSpec as P

MESH = pl.DeviceIdType.MESH
F32 = jnp.float32
BF16 = jnp.bfloat16
GROUP = 4
STAT = 128


def dot(a, b):
    return jnp.dot(a, b, preferred_element_type=F32)


def dot_t(a, b):
    return lax.dot_general(a, b, (((1,), (1,)), ((), ())), preferred_element_type=F32)


def iota(shape, dim):
    return lax.broadcasted_iota(jnp.int32, shape, dim)


def kernel(
    len_hbm, hid_hbm, hid3_hbm, wuq_hbm, wqr_hbm, wuk_hbm, wuv_hbm, wo_hbm, ckv_hbm, kr_hbm,
    out_ref,
    len_s, hid_v, hid3_v, wuq_v, wqr_v, wuk_v, wuv_v, wo_v, ckv_v, kr_v,
    em_v, qall, sbuf, acc_src, r1, s2, keep_v, r2, y_src, yr1, yc, yr2, f_src, f_rcv,
    w_sem, ckv_sem, kr_sem, q_send, q_recv, a_send, a_recv, c_send, c_recv, y_send, y_recv,
):
    n_rows = ckv_hbm.shape[0]
    shard = ckv_hbm.shape[1]
    lat = ckv_hbm.shape[2]
    rope = kr_hbm.shape[1]
    nope = wuq_hbm.shape[1]
    n_pair = n_rows // 2
    n_group = n_pair // GROUP
    d_model = hid_hbm.shape[1]
    half_d = d_model // 2
    scale = 1.0 / math.sqrt(nope + rope)

    me = lax.axis_index("seq")
    x = lax.div(me, 2)
    c = lax.rem(me, 2)
    sib = 2 * x + (1 - c)
    cnt = 2 * (1 - x) + c
    far = 3 - me

    def load(src, dst, sem):
        return pltpu.make_async_copy(src, dst, sem)

    loads = {
        "hid": load(hid_hbm, hid_v, w_sem.at[0]),
        "wqr": load(wqr_hbm, wqr_v, w_sem.at[1]),
        "wuk": load(wuk_hbm, wuk_v, w_sem.at[2]),
        "len": load(len_hbm, len_s, w_sem.at[7]),
        "hid3": load(hid3_hbm, hid3_v, w_sem.at[8]),
    }
    n_part = 4
    part = wuq_hbm.shape[0] // n_part
    for i in range(n_part):
        rows = pl.ds(i * part, part)
        loads["wuq", i] = load(wuq_hbm.at[rows], wuq_v.at[rows], w_sem.at[3 + i])
    late = {
        "wuv": load(wuv_hbm, wuv_v, w_sem.at[9]),
        "wo": load(wo_hbm, wo_v, w_sem.at[10]),
    }

    def ckv_load(p):
        rows = pl.ds(2 * p, 2)
        return load(ckv_hbm.at[rows], ckv_v.at[rows], ckv_sem.at[p])

    def kr_load(p):
        rows = pl.ds(2 * p, 2)
        return load(kr_hbm.at[rows], kr_v.at[rows], kr_sem.at[p])

    for w in loads.values():
        w.start()

    barrier = pltpu.get_barrier_semaphore()
    for peer in (sib, cnt, far):
        pl.semaphore_signal(barrier, inc=1, device_id={"seq": peer}, device_id_type=MESH)

    def start_rows(p, carry):
        kr_load(p).start()
        ckv_load(p).start()
        return carry

    lax.fori_loop(0, n_pair // 2, start_rows, 0)
    for w in late.values():
        w.start()
    lax.fori_loop(n_pair // 2, n_pair, start_rows, 0)

    def remote(src, dst, send, recv, peer):
        return pltpu.make_async_remote_copy(
            src_ref=src, dst_ref=dst, send_sem=send, recv_sem=recv,
            device_id={"seq": peer}, device_id_type=MESH,
        )

    n_head = wqr_hbm.shape[0] // rope
    n_local = n_rows * n_head
    lane_h = iota((n_rows, 4 * nope), 1) % n_head
    spread = (iota((nope, n_head * nope), 1) // n_head == iota((nope, n_head * nope), 0)).astype(F32).astype(BF16)
    loads["hid"].wait()
    for k in range(d_model // nope):
        wide = dot(hid_v[:, k * nope:(k + 1) * nope], spread)
        for h in range(n_head):
            em_v[h * n_rows:(h + 1) * n_rows, k * n_head * nope:(k + 1) * n_head * nope] = jnp.where(
                lane_h == h, wide, 0.0).astype(BF16)

    def row_of(r):
        j = (r // 4) % 2
        return 2 * (r // 8) + j + x - 2 * j * x

    loads["wqr"].wait()
    q_r = dot_t(hid_v[...], wqr_v[...]).astype(BF16)
    r_id = iota((n_local, n_rows), 0)
    rep = (iota((n_local, n_rows), 1) == row_of(r_id)).astype(F32).astype(BF16)
    q_r = dot(rep, q_r)
    q_r = jnp.where(iota((n_local, n_head * rope), 1) // rope == iota((n_local, n_head * rope), 0) % 4, q_r, 0.0)
    fold = (iota((n_head * rope, STAT), 0) % rope == iota((n_head * rope, STAT), 1)).astype(F32).astype(BF16)
    q_r = dot(q_r.astype(BF16), fold).astype(BF16)
    for p in range(n_pair):
        qall[me, p, :, lat:lat + STAT] = q_r[8 * p:8 * p + 8]
    r_id = iota((n_local, n_local), 0)
    col = iota((n_local, n_local), 1)
    perm = (col == (r_id % 4) * n_rows + row_of(r_id)).astype(F32).astype(BF16)
    r_h = iota((n_local, nope), 0) % 4

    for name in ("wuk", "len", "hid3"):
        loads[name].wait()
    for i in range(n_part):
        loads["wuq", i].wait()
        rows = slice(i * part, (i + 1) * part)
        term = dot(em_v[:, rows], wuq_v[rows, :])
        q_n = term if i == 0 else q_n + term
    q_p = dot(perm, q_n.astype(BF16))
    q_wide = jnp.concatenate([jnp.where(r_h == h, q_p, 0.0).astype(BF16) for h in range(n_head)], axis=1)
    q_l = dot(q_wide, wuk_v[...]).astype(BF16)
    for p in range(n_pair):
        qall[me, p, :, 0:lat] = q_l[8 * p:8 * p + 8]

    pl.semaphore_wait(barrier, 3)

    chunks = ((0, 3), (3, 7), (7, n_pair))

    def q_copy(kind, g):
        slot, peer = ((me, sib), (me, cnt), (me, far) if g == 0 else (cnt, sib))[kind]
        first, last = chunks[g]
        rows = qall.at[slot, first:last]
        return remote(rows, rows, q_send.at[kind], q_recv.at[kind, g], peer)

    def q_forward(g):
        q_copy(1, g).wait_recv()
        q_copy(2, g).start()

    for kind in (1, 2, 0):
        q_copy(kind, 0).start()
    q_copy(1, 1).start()
    q_copy(0, 1).start()

    upper8 = iota((8, lat + STAT), 0) < 4

    def scores(p):
        tiles = [qall[s, p].astype(F32) for s in range(4)]
        q_even = jnp.concatenate([jnp.where(upper8, tiles[0], tiles[2]), jnp.where(upper8, tiles[1], tiles[3])], axis=0)
        q_odd = jnp.concatenate([jnp.where(upper8, tiles[2], tiles[0]), jnp.where(upper8, tiles[3], tiles[1])], axis=0)
        for i, q in enumerate((q_even, q_odd)):
            q = q.astype(BF16)
            b = 2 * p + i
            s = dot_t(q[:, :lat], ckv_v[b]) + dot(q[:, lat:lat + rope], kr_v[b])
            sbuf[p % 2, i] = s

    def wait_rows(p):
        kr_load(p).wait()
        ckv_load(p).wait()

    stat_lane = iota((16, STAT), 1) < STAT // 2

    def attend(p):
        for i in (0, 1):
            b = 2 * p + i
            s = sbuf[p % 2, i] * scale
            pos = me * shard + iota(s.shape, 1)
            s = jnp.where(pos < len_s[b], s, -jnp.inf)
            m = jnp.max(s, axis=1, keepdims=True)
            e = jnp.exp(s - jnp.where(m > -jnp.inf, m, 0.0))
            l = jnp.sum(e, axis=1, keepdims=True)
            acc = dot(e.astype(BF16), ckv_v[b])
            stat = jnp.where(stat_lane, m, l)
            for k in (0, 1):
                acc_src[k, b, :, 0:lat] = acc[8 * k:8 * k + 8]
                acc_src[k, b, :, lat:lat + STAT] = stat[8 * k:8 * k + 8]

    def pair_copy(p):
        rows = pl.ds(2 * p, 2)
        return remote(acc_src.at[1 - c, rows], r1.at[rows], a_send, a_recv.at[p], sib)

    def chip_copy(p):
        return remote(s2.at[p], r2.at[p], c_send, c_recv.at[p], cnt)

    def merge(a, b):
        m1, l1 = a[:, lat:lat + 1], a[:, lat + STAT // 2:lat + STAT // 2 + 1]
        m2, l2 = b[:, lat:lat + 1], b[:, lat + STAT // 2:lat + STAT // 2 + 1]
        m = jnp.maximum(m1, m2)
        shift = jnp.where(m > -jnp.inf, m, 0.0)
        w1, w2 = jnp.exp(m1 - shift), jnp.exp(m2 - shift)
        return w1 * a[:, :lat] + w2 * b[:, :lat], m, w1 * l1 + w2 * l2

    stat_lane8 = iota((8, STAT), 1) < STAT // 2

    def merge_pair(p):
        both = []
        for i in (0, 1):
            acc, m, l = merge(acc_src[c, 2 * p + i], r1[2 * p + i])
            both.append((acc, jnp.where(stat_lane8, m, l)))
        for k, (lo, hi) in enumerate(((0, lat), (lat, lat + STAT))):
            upper = upper8[:, lo:hi]
            zero = jnp.where(upper, both[0][k], both[1][k])
            one = jnp.where(upper, both[1][k], both[0][k])
            keep_v[p, :, lo:hi] = jnp.where(x == 0, zero, one)
            s2[p, :, lo:hi] = jnp.where(x == 0, one, zero)

    def o_rows(p):
        acc, _, l = merge(keep_v[p], r2[p])
        return acc / l

    n_out = 8 * GROUP

    def project(g):
        o_lat = jnp.concatenate([o_rows(GROUP * g + i) for i in range(GROUP)], axis=0).astype(BF16)
        head = iota((n_out, nope), 0) % 4
        wide = jnp.concatenate(
            [jnp.where(head == h, dot(o_lat, wuv_v[h]), 0.0).astype(BF16) for h in range(n_head)], axis=1)
        r = iota((8, n_out), 1)
        gather = (iota((8, n_out), 0) == row_of(r)).astype(F32).astype(BF16)
        o_val = dot(gather, wide).astype(BF16)
        for k in (0, 1):
            y_src[g, k] = dot(o_val, wo_v[:, k * half_d:(k + 1) * half_d])

    def y_copy(kind, g):
        if kind == 0:
            src, dst, peer = y_src.at[g, 1 - c], yr1.at[g], sib
        elif kind == 1:
            src, dst, peer = yc.at[g], yr2.at[g], cnt
        else:
            src, dst, peer = f_src.at[g], f_rcv.at[g], sib
        return remote(src, dst, y_send.at[kind], y_recv.at[kind, g], peer)

    def y_chip(g):
        y_copy(0, g).wait_recv()
        yc[g] = y_src[g, c] + yr1[g]
        y_copy(1, g).start()

    def y_final(g):
        y_copy(1, g).wait_recv()
        hid = hid3_v[g, :, pl.ds(pl.multiple_of(c * half_d, half_d), half_d)].astype(F32)
        f_src[g] = (hid + (yc[g] + yr2[g])).astype(BF16)
        y_copy(2, g).start()

    def store(g):
        y_copy(2, g).wait_recv()
        mine, other = f_src[g].astype(F32), f_rcv[g].astype(F32)
        out_ref[g, :, 0:half_d] = jnp.where(c == 0, mine, other).astype(BF16)
        out_ref[g, :, half_d:d_model] = jnp.where(c == 0, other, mine).astype(BF16)

    def step(js, merges=(), groups=()):
        for j in js:
            wait_rows(j)
        for p in merges:
            pair_copy(p).wait_recv()
        for g in groups:
            for i in range(GROUP):
                chip_copy(GROUP * g + i).wait_recv()
        for j in js:
            scores(j)
            attend(j - 1)
        for p in merges:
            merge_pair(p)
        for g in groups:
            project(g)
        for j in js:
            pair_copy(j - 1).start()
        for p in merges:
            chip_copy(p).start()
        for g in groups:
            y_copy(0, g).start()

    for kind in range(3):
        q_copy(kind, 0).wait_recv()
    q_copy(1, 2).start()
    q_copy(0, 2).start()
    wait_rows(0)
    scores(0)
    q_forward(1)
    step((1, 2))
    q_copy(0, 1).wait_recv()
    q_copy(2, 1).wait_recv()
    step((3, 4))
    q_forward(2)
    step((5, 6), (0, 1))
    q_copy(0, 2).wait_recv()
    q_copy(2, 2).wait_recv()
    step((7, 8), (2, 3))
    step((9, 10), (4, 5))
    step((11,), (6, 7))
    for w in late.values():
        w.wait()
    step((12,), (8, 9), (0,))
    step((13,), (10,))
    y_chip(0)
    step((14,), (11,))
    step((15,), (12,), (1,))
    attend(n_pair - 1)
    pair_copy(n_pair - 1).start()

    def last_merge(p):
        pair_copy(p).wait_recv()
        merge_pair(p)
        chip_copy(p).start()

    def last_project(g):
        for i in range(GROUP):
            chip_copy(GROUP * g + i).wait_recv()
        project(g)
        y_copy(0, g).start()

    last_merge(13)
    last_merge(14)
    last_merge(15)
    y_chip(1)
    y_final(0)
    last_project(2)
    y_chip(2)
    last_project(3)
    y_final(1)
    y_chip(3)
    store(0)
    y_final(2)
    store(1)
    store(2)
    y_final(3)
    for kind in range(3):
        remote(qall.at[me], qall.at[me], q_send.at[kind], q_recv.at[kind, 0], sib).wait_send()
        whole = (yr1, yr2, f_rcv)[kind]
        remote(whole, whole, y_send.at[kind], y_recv.at[kind, 0], sib).wait_send()
    remote(r1, r1, a_send, a_recv.at[0], sib).wait_send()
    remote(r2, r2, c_send, c_recv.at[0], cnt).wait_send()
    store(3)


def solution(mesh):
    row_spec = P('batch', None)
    cache_spec = P('batch', 'seq', None)
    in_specs = (row_spec, P('batch'), cache_spec, cache_spec, P(None, 'seq', None), P(None, 'seq', None), P('seq', None, None), P('seq', None, None), P('seq', None, None))

    def mla_step(hidden, lengths, c_kv, k_rope, w_uq, w_qr, w_uk, w_uv, w_o):
        n_rows, d_model = hidden.shape
        _, shard, lat = c_kv.shape
        rope = k_rope.shape[2]
        n_head, nope = w_uq.shape[1], w_uq.shape[2]
        n_pair = n_rows // 2
        n_group = n_pair // GROUP
        wide = lat + STAT
        half = d_model // 2
        hid3 = hidden.reshape(n_group, 8, d_model)
        operands = (
            lengths,
            hidden,
            hid3,
            w_uq.reshape(d_model * n_head, nope),
            jnp.transpose(w_qr, (1, 2, 0)).reshape(n_head * rope, d_model),
            w_uk.reshape(n_head * nope, lat),
            w_uv,
            w_o.reshape(n_head * w_o.shape[1], d_model),
            c_kv,
            jnp.transpose(k_rope, (0, 2, 1)),
        )
        operands = tuple(pltpu.with_memory_space_constraint(a, pltpu.HBM) for a in operands)
        vm = pltpu.VMEM
        dma = pltpu.SemaphoreType.DMA
        out = pl.pallas_call(
            kernel,
            out_shape=jax.ShapeDtypeStruct((n_group, 8, d_model), BF16),
            in_specs=[pl.BlockSpec(memory_space=pltpu.HBM)] * len(operands),
            out_specs=pl.BlockSpec(memory_space=pltpu.VMEM),
            scratch_shapes=[
                pltpu.SMEM((n_rows,), jnp.int32),
                vm(hidden.shape, BF16),
                vm(hid3.shape, BF16),
                vm(operands[3].shape, BF16),
                vm(operands[4].shape, BF16),
                vm(operands[5].shape, BF16),
                vm(operands[6].shape, BF16),
                vm(operands[7].shape, BF16),
                vm(c_kv.shape, BF16),
                vm(operands[9].shape, BF16),
                vm((n_head * n_rows, n_head * d_model), BF16),
                vm((4, n_pair, 8, wide), BF16),
                vm((2, 2, 16, shard), F32),
                vm((2, n_rows, 8, wide), F32),
                vm((n_rows, 8, wide), F32),
                vm((n_pair, 8, wide), F32),
                vm((n_pair, 8, wide), F32),
                vm((n_pair, 8, wide), F32),
                vm((n_group, 2, 8, half), F32),
                vm((n_group, 8, half), F32),
                vm((n_group, 8, half), F32),
                vm((n_group, 8, half), F32),
                vm((n_group, 8, half), BF16),
                vm((n_group, 8, half), BF16),
                dma((11,)),
                dma((n_pair,)),
                dma((n_pair,)),
                dma((3,)),
                dma((3, 3)),
                dma(()),
                dma((n_pair,)),
                dma(()),
                dma((n_pair,)),
                dma((3,)),
                dma((3, n_group)),
            ],
            compiler_params=pltpu.CompilerParams(
                collective_id=0, has_side_effects=True, vmem_limit_bytes=50 * 1024 * 1024,
            ),
            name="mla_decode",
        )(*operands)
        return out.reshape(n_rows, d_model)

    return jax.shard_map(mla_step, mesh=mesh, in_specs=in_specs, out_specs=row_spec, check_vma=False)
```

```python
import math

import jax
import jax.numpy as jnp
from jax import lax
from jax.experimental import pallas as pl
from jax.experimental.pallas import tpu as pltpu
from jax.sharding import PartitionSpec as P

MESH = pl.DeviceIdType.MESH
F32 = jnp.float32
BF16 = jnp.bfloat16
GROUP = 4
STAT = 128


def dot(a, b):
    return jnp.dot(a, b, preferred_element_type=F32)


def dot_t(a, b):
    return lax.dot_general(a, b, (((1,), (1,)), ((), ())), preferred_element_type=F32)


def iota(shape, dim):
    return lax.broadcasted_iota(jnp.int32, shape, dim)


def kernel(
    len_hbm, hid_hbm, hid3_hbm, wuq_hbm, wqr_hbm, wuk_hbm, wuv_hbm, wo_hbm, ckv_hbm, kr_hbm,
    out_ref,
    len_s, hid_v, hid3_v, hid_r, wuq_v, wqr_v, wuk_v, wuv_v, wo_v, ckv_v, kr_v,
    em_v, qall, sbuf, acc_src, r1, s2, keep_v, r2, y_src, yr1, yc, yr2, f_src, f_rcv, y_last,
    w_sem, ckv_sem, kr_sem, q_send, q_recv, a_send, a_recv, c_send, c_recv, y_send, y_recv, f_send, f_recv, l_send, l_recv,
):
    n_rows = ckv_hbm.shape[0]
    shard = ckv_hbm.shape[1]
    lat = ckv_hbm.shape[2]
    rope = kr_hbm.shape[1]
    nope = wuq_hbm.shape[1]
    n_pair = n_rows // 2
    n_group = n_pair // GROUP
    d_model = hid_hbm.shape[1]
    half_d = d_model // 2
    scale = 1.0 / math.sqrt(nope + rope)

    me = lax.axis_index("seq")
    x = lax.div(me, 2)
    c = lax.rem(me, 2)
    sib = 2 * x + (1 - c)
    cnt = 2 * (1 - x) + c
    far = 3 - me

    def load(src, dst, sem):
        return pltpu.make_async_copy(src, dst, sem)

    hid_load = load(hid_hbm, hid_v, w_sem.at[0])
    early = [load(src, dst, w_sem.at[1 + i]) for i, (src, dst) in enumerate((
        (wqr_hbm, wqr_v), (wuk_hbm, wuk_v), (len_hbm, len_s), (hid3_hbm, hid3_v), (wuq_hbm, wuq_v)))]
    late = [load(src, dst, w_sem.at[6 + i]) for i, (src, dst) in enumerate(((wuv_hbm, wuv_v), (wo_hbm, wo_v)))]
    spans = ((0, 1), (1, 3), (3, 7), (7, 11), (11, n_pair))

    def row_loads(i):
        rows = slice(2 * spans[i][0], 2 * spans[i][1])
        return (load(kr_hbm.at[rows], kr_v.at[rows], kr_sem.at[i]), load(ckv_hbm.at[rows], ckv_v.at[rows], ckv_sem.at[i]))

    for w in (hid_load, *early):
        w.start()

    barrier = pltpu.get_barrier_semaphore()
    for peer in (sib, cnt, far):
        pl.semaphore_signal(barrier, inc=1, device_id={"seq": peer}, device_id_type=MESH)

    for i in range(len(spans)):
        for w in row_loads(i):
            w.start()
        if i == 2:
            for w in late:
                w.start()

    def remote(src, dst, send, recv, peer):
        return pltpu.make_async_remote_copy(
            src_ref=src, dst_ref=dst, send_sem=send, recv_sem=recv,
            device_id={"seq": peer}, device_id_type=MESH,
        )

    n_head = wqr_hbm.shape[0] // rope
    n_local = n_rows * n_head
    def row_of(r):
        j = (r // 4) % 2
        return 2 * (r // 8) + j + x - 2 * j * x

    r_h = iota((n_local, nope), 0) % 4
    same_head = iota((n_local, n_head * nope), 1) % n_head == iota((n_local, n_head * nope), 0) % 4
    spread = (iota((nope, n_head * nope), 1) // n_head == iota((nope, n_head * nope), 0)).astype(F32).astype(BF16)
    rep = (iota((n_local, n_rows), 1) == row_of(iota((n_local, n_rows), 0))).astype(F32).astype(BF16)
    fold = (iota((n_head * rope, STAT), 0) % rope == iota((n_head * rope, STAT), 1)).astype(F32).astype(BF16)
    hid_load.wait()
    hid_r[...] = dot(rep, hid_v[...]).astype(BF16)
    for k in range(d_model // nope):
        wide = dot(hid_r[:, k * nope:(k + 1) * nope], spread)
        em_v[:, k * n_head * nope:(k + 1) * n_head * nope] = jnp.where(same_head, wide, 0.0).astype(BF16)
    for w in early:
        w.wait()
    q_r = dot_t(hid_r[...], wqr_v[...])
    q_n = dot(em_v[...], wuq_v[...])
    q_r = jnp.where(iota((n_local, n_head * rope), 1) // rope == iota((n_local, n_head * rope), 0) % 4, q_r, 0.0)
    q_r = dot(q_r.astype(BF16), fold).astype(BF16)
    q_wide = jnp.concatenate([jnp.where(r_h == h, q_n, 0.0).astype(BF16) for h in range(n_head)], axis=1)
    q_l = dot(q_wide, wuk_v[...]).astype(BF16)
    for p in range(n_pair):
        qall[me, p, :, 0:lat] = q_l[8 * p:8 * p + 8]
        qall[me, p, :, lat:lat + STAT] = q_r[8 * p:8 * p + 8]

    pl.semaphore_wait(barrier, 3)

    chunks = ((0, 1), (1, 3), (3, 7), (7, n_pair))
    last_chunk = len(chunks) - 1

    def q_copy(kind, g):
        forward = g == last_chunk and kind == 1
        slot, peer = ((me, cnt), (cnt, sib) if forward else (me, far), (me, sib))[kind]
        rows = qall.at[slot, chunks[g][0]:chunks[g][1]]
        return remote(rows, rows, q_send, q_recv.at[g + 1 if g == last_chunk and kind == 0 else g], peer)

    def q_wait(g):
        rows = qall.at[0:2 if g == last_chunk else 3, chunks[g][0]:chunks[g][1]]
        remote(rows, rows, q_send, q_recv.at[g], sib).wait_recv()

    for g in range(last_chunk):
        for kind in range(3):
            q_copy(kind, g).start()

    upper8 = iota((8, lat + STAT), 0) < 4

    def scores(p):
        tiles = [qall[s, p].astype(F32) for s in range(4)]
        q_even = jnp.concatenate([jnp.where(upper8, tiles[0], tiles[2]), jnp.where(upper8, tiles[1], tiles[3])], axis=0)
        q_odd = jnp.concatenate([jnp.where(upper8, tiles[2], tiles[0]), jnp.where(upper8, tiles[3], tiles[1])], axis=0)
        for i, q in enumerate((q_even, q_odd)):
            q = q.astype(BF16)
            b = 2 * p + i
            s = dot_t(q[:, :lat], ckv_v[b]) + dot(q[:, lat:lat + rope], kr_v[b])
            sbuf[p % 2, i] = s

    def wait_rows(p):
        for i, span in enumerate(spans):
            if p == span[0]:
                for w in row_loads(i):
                    w.wait()

    stat_lane = iota((16, STAT), 1) < STAT // 2

    def attend(p):
        for i in (0, 1):
            b = 2 * p + i
            s = sbuf[p % 2, i] * scale
            pos = me * shard + iota(s.shape, 1)
            s = jnp.where(pos < len_s[b], s, -jnp.inf)
            m = jnp.max(s, axis=1, keepdims=True)
            e = jnp.exp(s - jnp.where(m > -jnp.inf, m, 0.0))
            l = jnp.sum(e, axis=1, keepdims=True)
            acc = dot(e.astype(BF16), ckv_v[b])
            stat = jnp.where(stat_lane, m, l)
            for k in (0, 1):
                acc_src[k, b, :, 0:lat] = acc[8 * k:8 * k + 8]
                acc_src[k, b, :, lat:lat + STAT] = stat[8 * k:8 * k + 8]

    sends = ((0, 1), (2, 3), (4, 5), (6, 7), (8, 9), (10,), (11,), (12,), (13,), (14,), (15,))

    def pair_copy(ps):
        rows = slice(2 * ps[0], 2 * ps[-1] + 2)
        return remote(acc_src.at[1 - c, rows], r1.at[rows], a_send, a_recv.at[sends.index(ps)], sib)

    def chip_copy(ps):
        rows = slice(ps[0], ps[-1] + 1)
        return remote(s2.at[rows], r2.at[rows], c_send, c_recv.at[ps[0] // GROUP], cnt)

    def chip_wait(g):
        rows = r2.at[GROUP * g:GROUP * (g + 1)]
        remote(rows, rows, c_send, c_recv.at[g], cnt).wait_recv()

    def merge(a, b):
        m1, l1 = a[:, lat:lat + 1], a[:, lat + STAT // 2:lat + STAT // 2 + 1]
        m2, l2 = b[:, lat:lat + 1], b[:, lat + STAT // 2:lat + STAT // 2 + 1]
        m = jnp.maximum(m1, m2)
        shift = jnp.where(m > -jnp.inf, m, 0.0)
        w1, w2 = jnp.exp(m1 - shift), jnp.exp(m2 - shift)
        return w1 * a[:, :lat] + w2 * b[:, :lat], m, w1 * l1 + w2 * l2

    stat_lane8 = iota((8, STAT), 1) < STAT // 2

    def merge_pair(p):
        both = []
        for i in (0, 1):
            acc, m, l = merge(acc_src[c, 2 * p + i], r1[2 * p + i])
            both.append((acc, jnp.where(stat_lane8, m, l)))
        for k, (lo, hi) in enumerate(((0, lat), (lat, lat + STAT))):
            upper = upper8[:, lo:hi]
            zero = jnp.where(upper, both[0][k], both[1][k])
            one = jnp.where(upper, both[1][k], both[0][k])
            keep_v[p, :, lo:hi] = jnp.where(x == 0, zero, one)
            s2[p, :, lo:hi] = jnp.where(x == 0, one, zero)

    def o_rows(p):
        acc, _, l = merge(keep_v[p], r2[p])
        return acc / l

    n_out = 8 * GROUP

    def project(g):
        o_lat = jnp.concatenate([o_rows(GROUP * g + i) for i in range(GROUP)], axis=0).astype(BF16)
        head = iota((n_out, nope), 0) % 4
        wide = []
        for h in range(0, n_head, 2):
            two = dot(o_lat, jnp.concatenate([wuv_v[h], wuv_v[h + 1]], axis=1))
            wide += [jnp.where(head == h + i, two[:, i * nope:(i + 1) * nope], 0.0).astype(BF16) for i in (0, 1)]
        wide = jnp.concatenate(wide, axis=1)
        r = iota((8, n_out), 1)
        gather = (iota((8, n_out), 0) == row_of(r)).astype(F32).astype(BF16)
        o_val = dot(gather, wide).astype(BF16)
        for k in (0, 1):
            y_src[g, k] = dot(o_val, wo_v[:, k * half_d:(k + 1) * half_d])

    def y_copy(kind, g):
        if kind == 0:
            return remote(y_src.at[g, 1 - c], yr1.at[g], y_send, y_recv.at[0, g], sib)
        return remote(yc.at[g], yr2.at[g], y_send, y_recv.at[1, g], cnt)

    def f_copy(g):
        return remote(f_src.at[g], f_rcv.at[g], f_send, f_recv, sib)

    def last_copy(i):
        return remote(yc.at[n_group - 1], y_last.at[i], l_send, l_recv, (sib, far)[i])

    def y_chip(g):
        y_copy(0, g).wait_recv()
        yc[g] = y_src[g, c] + yr1[g]
        y_copy(1, g).start()

    def hid_half(g, k):
        return hid3_v[g, :, pl.ds(pl.multiple_of(k * half_d, half_d), half_d)].astype(F32)

    def y_final(g):
        y_copy(1, g).wait_recv()
        f_src[g] = (hid_half(g, c) + (yc[g] + yr2[g])).astype(BF16)
        f_copy(g).start()

    def put(g, mine, other):
        out_ref[g, :, 0:half_d] = jnp.where(c == 0, mine, other).astype(BF16)
        out_ref[g, :, half_d:d_model] = jnp.where(c == 0, other, mine).astype(BF16)

    def step(js, merges=(), groups=()):
        for j in js:
            wait_rows(j)
        if merges:
            pair_copy(merges).wait_recv()
        for g in groups:
            chip_wait(g)
        for j in js:
            scores(j)
            attend(j - 1)
        for p in merges:
            merge_pair(p)
        for g in groups:
            project(g)
        pair_copy(tuple(j - 1 for j in js)).start()
        if merges:
            chip_copy(merges).start()
        for g in groups:
            y_copy(0, g).start()

    q_wait(0)
    for kind in (0, 2):
        q_copy(kind, last_chunk).start()
    wait_rows(0)
    scores(0)
    q_wait(1)
    step((1, 2))
    q_wait(2)
    step((3, 4))
    q_copy(0, last_chunk).wait_recv()
    q_copy(1, last_chunk).start()
    step((5, 6), (0, 1))
    q_wait(last_chunk)
    step((7, 8), (2, 3))
    step((9, 10), (4, 5))
    step((11,), (6, 7))
    for w in late:
        w.wait()
    step((12,), (8, 9), (0,))
    step((13,), (10,))
    y_chip(0)
    step((14,), (11,))
    step((15,), (12,))
    attend(n_pair - 1)
    pair_copy((n_pair - 1,)).start()

    def last_merge(p):
        pair_copy((p,)).wait_recv()
        merge_pair(p)
        chip_copy((p,)).start()

    def last_project(g):
        chip_wait(g)
        project(g)
        y_copy(0, g).start()

    last_merge(13)
    last_merge(14)
    last_merge(15)
    last_project(1)
    last_project(2)
    y_chip(1)
    y_final(0)
    last_project(3)
    y_chip(2)
    y_final(1)
    y_chip(3)
    for i in (0, 1):
        last_copy(i).start()
    y_final(2)
    some = f_rcv.at[0:n_group - 1]
    remote(some, some, f_send, f_recv, sib).wait_recv()
    for g in range(n_group - 1):
        put(g, f_src[g].astype(F32), f_rcv[g].astype(F32))
    remote(qall.at[0:3], qall.at[0:3], q_send, q_recv.at[0], sib).wait_send()
    remote(r1, r1, a_send, a_recv.at[0], sib).wait_send()
    remote(r2, r2, c_send, c_recv.at[0], cnt).wait_send()
    remote(some, some, f_send, f_recv, sib).wait_send()
    both = y_src.at[:, 0:2]
    remote(both, both, y_send, y_recv.at[0, 0], sib).wait_send()
    remote(y_last, y_last, l_send, l_recv, sib).wait_send()
    g = n_group - 1
    y_copy(1, g).wait_recv()
    remote(y_last, y_last, l_send, l_recv, sib).wait_recv()
    put(g, hid_half(g, c) + (yc[g] + yr2[g]), hid_half(g, 1 - c) + (y_last[0] + y_last[1]))


def solution(mesh):
    row_spec = P('batch', None)
    cache_spec = P('batch', 'seq', None)
    in_specs = (row_spec, P('batch'), cache_spec, cache_spec, P(None, 'seq', None), P(None, 'seq', None), P('seq', None, None), P('seq', None, None), P('seq', None, None))

    def mla_step(hidden, lengths, c_kv, k_rope, w_uq, w_qr, w_uk, w_uv, w_o):
        n_rows, d_model = hidden.shape
        _, shard, lat = c_kv.shape
        rope = k_rope.shape[2]
        n_head, nope = w_uq.shape[1], w_uq.shape[2]
        n_pair = n_rows // 2
        n_group = n_pair // GROUP
        wide = lat + STAT
        half = d_model // 2
        hid3 = hidden.reshape(n_group, 8, d_model)
        operands = (
            lengths,
            hidden,
            hid3,
            w_uq.reshape(d_model * n_head, nope),
            jnp.transpose(w_qr, (1, 2, 0)).reshape(n_head * rope, d_model),
            w_uk.reshape(n_head * nope, lat),
            w_uv,
            w_o.reshape(n_head * w_o.shape[1], d_model),
            c_kv,
            jnp.transpose(k_rope, (0, 2, 1)),
        )
        operands = tuple(pltpu.with_memory_space_constraint(a, pltpu.HBM) for a in operands)
        vm = pltpu.VMEM
        dma = pltpu.SemaphoreType.DMA
        out = pl.pallas_call(
            kernel,
            out_shape=jax.ShapeDtypeStruct((n_group, 8, d_model), BF16),
            in_specs=[pl.BlockSpec(memory_space=pltpu.HBM)] * len(operands),
            out_specs=pl.BlockSpec(memory_space=pltpu.VMEM),
            scratch_shapes=[
                pltpu.SMEM((n_rows,), jnp.int32),
                vm(hidden.shape, BF16),
                vm(hid3.shape, BF16),
                vm((n_head * n_rows, d_model), BF16),
                vm(operands[3].shape, BF16),
                vm(operands[4].shape, BF16),
                vm(operands[5].shape, BF16),
                vm(operands[6].shape, BF16),
                vm(operands[7].shape, BF16),
                vm(c_kv.shape, BF16),
                vm(operands[9].shape, BF16),
                vm((n_head * n_rows, n_head * d_model), BF16),
                vm((4, n_pair, 8, wide), BF16),
                vm((2, 2, 16, shard), F32),
                vm((2, n_rows, 8, wide), F32),
                vm((n_rows, 8, wide), F32),
                vm((n_pair, 8, wide), F32),
                vm((n_pair, 8, wide), F32),
                vm((n_pair, 8, wide), F32),
                vm((n_group, 2, 8, half), F32),
                vm((n_group, 8, half), F32),
                vm((n_group, 8, half), F32),
                vm((n_group, 8, half), F32),
                vm((n_group, 8, half), BF16),
                vm((n_group, 8, half), BF16),
                vm((2, 8, half), F32),
                dma((8,)),
                dma((5,)),
                dma((5,)),
                dma(()),
                dma((5,)),
                dma(()),
                dma((11,)),
                dma(()),
                dma((n_group,)),
                dma(()),
                dma((2, n_group)),
                dma(()),
                dma(()),
                dma(()),
                dma(()),
            ],
            compiler_params=pltpu.CompilerParams(
                collective_id=0, has_side_effects=True, vmem_limit_bytes=52 * 1024 * 1024,
            ),
            name="mla_decode",
        )(*operands)
        return out.reshape(n_rows, d_model)

    return jax.shard_map(mla_step, mesh=mesh, in_specs=in_specs, out_specs=row_spec, check_vma=False)
```

```python
import math

import jax
import jax.numpy as jnp
from jax import lax
from jax.experimental import pallas as pl
from jax.experimental.pallas import tpu as pltpu
from jax.sharding import PartitionSpec as P

MESH = pl.DeviceIdType.MESH
F32 = jnp.float32
BF16 = jnp.bfloat16
GROUP = 4
STAT = 128


def dot(a, b):
    return jnp.dot(a, b, preferred_element_type=F32)


def dot_t(a, b):
    return lax.dot_general(a, b, (((1,), (1,)), ((), ())), preferred_element_type=F32)


def iota(shape, dim):
    return lax.broadcasted_iota(jnp.int32, shape, dim)


def kernel(
    len_hbm, hid_hbm, hid3_hbm, wuq_hbm, wqr_hbm, wuk_hbm, wuv_hbm, wo_hbm, ckv_hbm, kr_hbm,
    out_ref,
    len_s, hid_v, hid3_v, hid_r, wuq_v, wqr_v, wuk_v, wuv_v, wo_v, ckv_v, kr_v,
    em_v, qall, sbuf, acc_src, r1, s2, keep_v, r2, y_src, yr1, yc, yr2, f_src, f_rcv, y_last,
    w_sem, ckv_sem, kr_sem, q_send, q_recv, a_send, a_recv, c_send, c_recv, y_send, y_recv, f_send, f_recv, l_send, l_recv,
):
    n_rows = ckv_hbm.shape[0]
    shard = ckv_hbm.shape[1]
    lat = ckv_hbm.shape[2]
    rope = kr_hbm.shape[1]
    nope = wuq_hbm.shape[1]
    n_pair = n_rows // 2
    n_group = n_pair // GROUP
    d_model = hid_hbm.shape[1]
    half_d = d_model // 2
    scale = 1.0 / math.sqrt(nope + rope)

    me = lax.axis_index("seq")
    x = lax.div(me, 2)
    c = lax.rem(me, 2)
    sib = 2 * x + (1 - c)
    cnt = 2 * (1 - x) + c
    far = 3 - me

    def load(src, dst, sem):
        return pltpu.make_async_copy(src, dst, sem)

    hid_load = load(hid_hbm, hid_v, w_sem.at[0])
    early = [load(src, dst, w_sem.at[1 + i]) for i, (src, dst) in enumerate((
        (wqr_hbm, wqr_v), (wuk_hbm, wuk_v), (len_hbm, len_s), (hid3_hbm, hid3_v), (wuq_hbm, wuq_v)))]
    late = [load(src, dst, w_sem.at[6 + i]) for i, (src, dst) in enumerate(((wuv_hbm, wuv_v), (wo_hbm, wo_v)))]
    spans = ((0, 1), (1, 3), (3, 7), (7, 11), (11, n_pair))

    def row_loads(i):
        rows = slice(2 * spans[i][0], 2 * spans[i][1])
        return (load(kr_hbm.at[rows], kr_v.at[rows], kr_sem.at[i]), load(ckv_hbm.at[rows], ckv_v.at[rows], ckv_sem.at[i]))

    for w in (hid_load, *early):
        w.start()

    barrier = pltpu.get_barrier_semaphore()
    for peer in (sib, cnt, far):
        pl.semaphore_signal(barrier, inc=1, device_id={"seq": peer}, device_id_type=MESH)

    for i in range(len(spans)):
        for w in row_loads(i):
            w.start()
        if i == 2:
            for w in late:
                w.start()

    def remote(src, dst, send, recv, peer):
        return pltpu.make_async_remote_copy(
            src_ref=src, dst_ref=dst, send_sem=send, recv_sem=recv,
            device_id={"seq": peer}, device_id_type=MESH,
        )

    n_head = wqr_hbm.shape[0] // rope
    n_local = n_rows * n_head
    def row_of(r):
        j = (r // 4) % 2
        return 2 * (r // 8) + j + x - 2 * j * x

    r_h = iota((n_local, nope), 0) % 4
    same_head = iota((n_local, n_head * nope), 1) % n_head == iota((n_local, n_head * nope), 0) % 4
    spread = (iota((nope, n_head * nope), 1) // n_head == iota((nope, n_head * nope), 0)).astype(F32).astype(BF16)
    rep = (iota((n_local, n_rows), 1) == row_of(iota((n_local, n_rows), 0))).astype(F32).astype(BF16)
    fold = (iota((n_head * rope, STAT), 0) % rope == iota((n_head * rope, STAT), 1)).astype(F32).astype(BF16)
    hid_load.wait()
    hid_r[...] = dot(rep, hid_v[...]).astype(BF16)
    for k in range(d_model // nope):
        wide = dot(hid_r[:, k * nope:(k + 1) * nope], spread)
        em_v[:, k * n_head * nope:(k + 1) * n_head * nope] = jnp.where(same_head, wide, 0.0).astype(BF16)
    for w in early:
        w.wait()
    q_r = dot_t(hid_r[...], wqr_v[...])
    q_n = dot(em_v[...], wuq_v[...])
    q_r = jnp.where(iota((n_local, n_head * rope), 1) // rope == iota((n_local, n_head * rope), 0) % 4, q_r, 0.0)
    q_r = dot(q_r.astype(BF16), fold).astype(BF16)
    q_wide = jnp.concatenate([jnp.where(r_h == h, q_n, 0.0).astype(BF16) for h in range(n_head)], axis=1)
    q_l = dot(q_wide, wuk_v[...]).astype(BF16)
    for p in range(n_pair):
        qall[me, p, :, 0:lat] = q_l[8 * p:8 * p + 8]
        qall[me, p, :, lat:lat + STAT] = q_r[8 * p:8 * p + 8]

    pl.semaphore_wait(barrier, 3)

    chunks = ((0, 1), (1, 3), (3, 7), (7, 11), (11, n_pair))
    n_direct = 3

    def q_copy(kind, g):
        forward = g >= n_direct and kind == 1
        slot, peer = ((me, cnt), (cnt, sib) if forward else (me, far), (me, sib))[kind]
        rows = qall.at[slot, chunks[g][0]:chunks[g][1]]
        return remote(rows, rows, q_send, q_recv.at[g + 2 if g >= n_direct and kind == 0 else g], peer)

    def q_wait(g):
        rows = qall.at[0:2 if g >= n_direct else 3, chunks[g][0]:chunks[g][1]]
        remote(rows, rows, q_send, q_recv.at[g], sib).wait_recv()

    def q_forward(g):
        q_copy(0, g).wait_recv()
        q_copy(1, g).start()

    for g in range(n_direct):
        for kind in range(3):
            q_copy(kind, g).start()

    upper8 = iota((8, lat + STAT), 0) < 4

    def scores(p):
        tiles = [qall[s, p].astype(F32) for s in range(4)]
        q_even = jnp.concatenate([jnp.where(upper8, tiles[0], tiles[2]), jnp.where(upper8, tiles[1], tiles[3])], axis=0)
        q_odd = jnp.concatenate([jnp.where(upper8, tiles[2], tiles[0]), jnp.where(upper8, tiles[3], tiles[1])], axis=0)
        for i, q in enumerate((q_even, q_odd)):
            q = q.astype(BF16)
            b = 2 * p + i
            s = dot_t(q[:, :lat], ckv_v[b]) + dot(q[:, lat:lat + rope], kr_v[b])
            sbuf[p % 2, i] = s

    def wait_rows(p):
        for i, span in enumerate(spans):
            if p == span[0]:
                for w in row_loads(i):
                    w.wait()

    stat_lane = iota((16, STAT), 1) < STAT // 2

    def attend(p):
        for i in (0, 1):
            b = 2 * p + i
            s = sbuf[p % 2, i] * scale
            pos = me * shard + iota(s.shape, 1)
            s = jnp.where(pos < len_s[b], s, -jnp.inf)
            m = jnp.max(s, axis=1, keepdims=True)
            e = jnp.exp(s - jnp.where(m > -jnp.inf, m, 0.0))
            l = jnp.sum(e, axis=1, keepdims=True)
            acc = dot(e.astype(BF16), ckv_v[b])
            stat = jnp.where(stat_lane, m, l)
            for k in (0, 1):
                acc_src[k, b, :, 0:lat] = acc[8 * k:8 * k + 8]
                acc_src[k, b, :, lat:lat + STAT] = stat[8 * k:8 * k + 8]

    sends = ((0, 1), (2, 3), (4, 5), (6, 7), (8, 9), (10, 11), (12,), (13,), (14,), (15,))

    def pair_copy(ps):
        rows = slice(2 * ps[0], 2 * ps[-1] + 2)
        return remote(acc_src.at[1 - c, rows], r1.at[rows], a_send, a_recv.at[sends.index(ps)], sib)

    def chip_copy(ps):
        rows = slice(ps[0], ps[-1] + 1)
        return remote(s2.at[rows], r2.at[rows], c_send, c_recv.at[ps[0] // GROUP], cnt)

    def chip_wait(g):
        rows = r2.at[GROUP * g:GROUP * (g + 1)]
        remote(rows, rows, c_send, c_recv.at[g], cnt).wait_recv()

    def merge(a, b):
        m1, l1 = a[:, lat:lat + 1], a[:, lat + STAT // 2:lat + STAT // 2 + 1]
        m2, l2 = b[:, lat:lat + 1], b[:, lat + STAT // 2:lat + STAT // 2 + 1]
        m = jnp.maximum(m1, m2)
        shift = jnp.where(m > -jnp.inf, m, 0.0)
        w1, w2 = jnp.exp(m1 - shift), jnp.exp(m2 - shift)
        return w1 * a[:, :lat] + w2 * b[:, :lat], m, w1 * l1 + w2 * l2

    stat_lane8 = iota((8, STAT), 1) < STAT // 2

    def merge_pair(p):
        both = []
        for i in (0, 1):
            acc, m, l = merge(acc_src[c, 2 * p + i], r1[2 * p + i])
            both.append((acc, jnp.where(stat_lane8, m, l)))
        for k, (lo, hi) in enumerate(((0, lat), (lat, lat + STAT))):
            upper = upper8[:, lo:hi]
            zero = jnp.where(upper, both[0][k], both[1][k])
            one = jnp.where(upper, both[1][k], both[0][k])
            keep_v[p, :, lo:hi] = jnp.where(x == 0, zero, one)
            s2[p, :, lo:hi] = jnp.where(x == 0, one, zero)

    def o_rows(p):
        acc, _, l = merge(keep_v[p], r2[p])
        return acc / l

    n_out = 8 * GROUP

    def project(g, split=False):
        o_lat = jnp.concatenate([o_rows(GROUP * g + i) for i in range(GROUP)], axis=0).astype(BF16)
        head = iota((n_out, nope), 0) % 4
        wide = []
        for h in range(0, n_head, 2):
            two = dot(o_lat, jnp.concatenate([wuv_v[h], wuv_v[h + 1]], axis=1))
            wide += [jnp.where(head == h + i, two[:, i * nope:(i + 1) * nope], 0.0).astype(BF16) for i in (0, 1)]
        wide = jnp.concatenate(wide, axis=1)
        r = iota((8, n_out), 1)
        gather = (iota((8, n_out), 0) == row_of(r)).astype(F32).astype(BF16)
        o_val = dot(gather, wide).astype(BF16)
        if not split:
            for k in (0, 1):
                y_src[g, k] = dot(o_val, wo_v[:, k * half_d:(k + 1) * half_d])
            return
        for k in (1 - c, c):
            y_src[g, k] = dot(o_val, wo_v[:, pl.ds(pl.multiple_of(k * half_d, half_d), half_d)])
            if k is not c:
                y_copy(0, g).start()

    def y_copy(kind, g):
        if kind == 0:
            return remote(y_src.at[g, 1 - c], yr1.at[g], y_send, y_recv.at[0, g], sib)
        return remote(yc.at[g], yr2.at[g], y_send, y_recv.at[1, g], cnt)

    def f_copy(g):
        return remote(f_src.at[g], f_rcv.at[g], f_send, f_recv, sib)

    def last_copy(i):
        return remote(yc.at[n_group - 1], y_last.at[i], l_send, l_recv, (sib, far)[i])

    def y_chip(g):
        y_copy(0, g).wait_recv()
        yc[g] = y_src[g, c] + yr1[g]
        y_copy(1, g).start()

    def hid_half(g, k):
        return hid3_v[g, :, pl.ds(pl.multiple_of(k * half_d, half_d), half_d)].astype(F32)

    def y_final(g):
        y_copy(1, g).wait_recv()
        f_src[g] = (hid_half(g, c) + (yc[g] + yr2[g])).astype(BF16)
        f_copy(g).start()

    def put(g, mine, other):
        out_ref[g, :, 0:half_d] = jnp.where(c == 0, mine, other).astype(BF16)
        out_ref[g, :, half_d:d_model] = jnp.where(c == 0, other, mine).astype(BF16)

    def step(js, merges=(), groups=()):
        for j in js:
            wait_rows(j)
        if merges:
            pair_copy(merges).wait_recv()
        for g in groups:
            chip_wait(g)
        for j in js:
            scores(j)
            attend(j - 1)
        for p in merges:
            merge_pair(p)
        for g in groups:
            project(g)
        pair_copy(tuple(j - 1 for j in js)).start()
        if merges:
            chip_copy(merges).start()
        for g in groups:
            y_copy(0, g).start()

    q_wait(0)
    for g in range(n_direct, len(chunks)):
        for kind in (0, 2):
            q_copy(kind, g).start()
    wait_rows(0)
    scores(0)
    q_wait(1)
    step((1, 2))
    q_wait(2)
    step((3, 4))
    q_forward(3)
    step((5, 6), (0, 1))
    q_forward(4)
    q_wait(3)
    step((7, 8), (2, 3))
    step((9, 10), (4, 5))
    q_wait(4)
    step((11, 12), (6, 7))
    for w in late:
        w.wait()
    step((13,), (8, 9))
    step((14,), (10, 11), (0,))
    step((15,), (12,))
    attend(n_pair - 1)
    pair_copy((n_pair - 1,)).start()

    def last_merge(ps):
        pair_copy(ps).wait_recv()
        for p in ps:
            merge_pair(p)
        chip_copy(ps).start()

    def last_project(g):
        chip_wait(g)
        project(g, g == n_group - 1)
        if g < n_group - 1:
            y_copy(0, g).start()

    last_merge((13,))
    last_merge((14,))
    last_merge((15,))
    last_project(1)
    y_chip(0)
    last_project(2)
    y_chip(1)
    y_final(0)
    y_chip(2)
    last_project(3)
    y_chip(3)
    for i in (0, 1):
        last_copy(i).start()
    y_final(1)
    y_final(2)
    some = f_rcv.at[0:n_group - 1]
    remote(some, some, f_send, f_recv, sib).wait_recv()
    for g in range(n_group - 1):
        put(g, f_src[g].astype(F32), f_rcv[g].astype(F32))
    remote(qall.at[0:3], qall.at[0:3], q_send, q_recv.at[0], sib).wait_send()
    remote(r1, r1, a_send, a_recv.at[0], sib).wait_send()
    remote(r2, r2, c_send, c_recv.at[0], cnt).wait_send()
    remote(some, some, f_send, f_recv, sib).wait_send()
    both = y_src.at[:, 0:2]
    remote(both, both, y_send, y_recv.at[0, 0], sib).wait_send()
    remote(y_last, y_last, l_send, l_recv, sib).wait_send()
    g = n_group - 1
    y_copy(1, g).wait_recv()
    remote(y_last, y_last, l_send, l_recv, sib).wait_recv()
    put(g, hid_half(g, c) + (yc[g] + yr2[g]), hid_half(g, 1 - c) + (y_last[0] + y_last[1]))


def solution(mesh):
    row_spec = P('batch', None)
    cache_spec = P('batch', 'seq', None)
    in_specs = (row_spec, P('batch'), cache_spec, cache_spec, P(None, 'seq', None), P(None, 'seq', None), P('seq', None, None), P('seq', None, None), P('seq', None, None))

    def mla_step(hidden, lengths, c_kv, k_rope, w_uq, w_qr, w_uk, w_uv, w_o):
        n_rows, d_model = hidden.shape
        _, shard, lat = c_kv.shape
        rope = k_rope.shape[2]
        n_head, nope = w_uq.shape[1], w_uq.shape[2]
        n_pair = n_rows // 2
        n_group = n_pair // GROUP
        wide = lat + STAT
        half = d_model // 2
        hid3 = hidden.reshape(n_group, 8, d_model)
        operands = (
            lengths,
            hidden,
            hid3,
            w_uq.reshape(d_model * n_head, nope),
            jnp.transpose(w_qr, (1, 2, 0)).reshape(n_head * rope, d_model),
            w_uk.reshape(n_head * nope, lat),
            w_uv,
            w_o.reshape(n_head * w_o.shape[1], d_model),
            c_kv,
            jnp.transpose(k_rope, (0, 2, 1)),
        )
        operands = tuple(pltpu.with_memory_space_constraint(a, pltpu.HBM) for a in operands)
        vm = pltpu.VMEM
        dma = pltpu.SemaphoreType.DMA
        out = pl.pallas_call(
            kernel,
            out_shape=jax.ShapeDtypeStruct((n_group, 8, d_model), BF16),
            in_specs=[pl.BlockSpec(memory_space=pltpu.HBM)] * len(operands),
            out_specs=pl.BlockSpec(memory_space=pltpu.VMEM),
            scratch_shapes=[
                pltpu.SMEM((n_rows,), jnp.int32),
                vm(hidden.shape, BF16),
                vm(hid3.shape, BF16),
                vm((n_head * n_rows, d_model), BF16),
                vm(operands[3].shape, BF16),
                vm(operands[4].shape, BF16),
                vm(operands[5].shape, BF16),
                vm(operands[6].shape, BF16),
                vm(operands[7].shape, BF16),
                vm(c_kv.shape, BF16),
                vm(operands[9].shape, BF16),
                vm((n_head * n_rows, n_head * d_model), BF16),
                vm((4, n_pair, 8, wide), BF16),
                vm((2, 2, 16, shard), F32),
                vm((2, n_rows, 8, wide), F32),
                vm((n_rows, 8, wide), F32),
                vm((n_pair, 8, wide), F32),
                vm((n_pair, 8, wide), F32),
                vm((n_pair, 8, wide), F32),
                vm((n_group, 2, 8, half), F32),
                vm((n_group, 8, half), F32),
                vm((n_group, 8, half), F32),
                vm((n_group, 8, half), F32),
                vm((n_group, 8, half), BF16),
                vm((n_group, 8, half), BF16),
                vm((2, 8, half), F32),
                dma((8,)),
                dma((5,)),
                dma((5,)),
                dma(()),
                dma((7,)),
                dma(()),
                dma((10,)),
                dma(()),
                dma((n_group,)),
                dma(()),
                dma((2, n_group)),
                dma(()),
                dma(()),
                dma(()),
                dma(()),
            ],
            compiler_params=pltpu.CompilerParams(
                collective_id=0, has_side_effects=True, vmem_limit_bytes=53 * 1024 * 1024,
            ),
            name="mla_decode",
        )(*operands)
        return out.reshape(n_rows, d_model)

    return jax.shard_map(mla_step, mesh=mesh, in_specs=in_specs, out_specs=row_spec, check_vma=False)
```

```python
import math

import jax
import jax.numpy as jnp
from jax import lax
from jax.experimental import pallas as pl
from jax.experimental.pallas import tpu as pltpu
from jax.sharding import PartitionSpec as P

MESH = pl.DeviceIdType.MESH
F32 = jnp.float32
BF16 = jnp.bfloat16
GROUP = 4
STAT = 128


def dot(a, b):
    return jnp.dot(a, b, preferred_element_type=F32)


def dot_t(a, b):
    return lax.dot_general(a, b, (((1,), (1,)), ((), ())), preferred_element_type=F32)


def iota(shape, dim):
    return lax.broadcasted_iota(jnp.int32, shape, dim)


def kernel(
    len_hbm, hid_hbm, hid3_hbm, wuq_hbm, wqr_hbm, wuk_hbm, wuv_hbm, wo_hbm, ckv_hbm, kr_hbm,
    out_ref,
    len_s, hid_v, hid3_v, hid_r, wuq_v, wqr_v, wuk_v, wuv_v, wo_v, ckv_v, kr_v,
    em_v, qall, sbuf, acc_src, r1, s2, keep_v, r2, y_src, yr1, yc, yr2, f_src, f_rcv, l_src, l_r1, l_sum, l_all,
    w_sem, ckv_sem, kr_sem, q_send, q_recv, a_send, a_recv, c_send, c_recv, y_send, y_recv, f_send, f_recv, l_send, l_recv,
):
    n_rows = ckv_hbm.shape[0]
    shard = ckv_hbm.shape[1]
    lat = ckv_hbm.shape[2]
    rope = kr_hbm.shape[1]
    nope = wuq_hbm.shape[1]
    n_pair = n_rows // 2
    d_model = hid_hbm.shape[1]
    half_d = d_model // 2
    scale = 1.0 / math.sqrt(nope + rope)

    me = lax.axis_index("seq")
    x = lax.div(me, 2)
    c = lax.rem(me, 2)
    sib = 2 * x + (1 - c)
    cnt = 2 * (1 - x) + c
    far = 3 - me

    def load(src, dst, sem):
        return pltpu.make_async_copy(src, dst, sem)

    hid_load = load(hid_hbm, hid_v, w_sem.at[0])
    early = [load(src, dst, w_sem.at[1 + i]) for i, (src, dst) in enumerate((
        (wqr_hbm, wqr_v), (wuk_hbm, wuk_v), (len_hbm, len_s), (hid3_hbm, hid3_v), (wuq_hbm, wuq_v)))]
    late = [load(src, dst, w_sem.at[6 + i]) for i, (src, dst) in enumerate(((wuv_hbm, wuv_v), (wo_hbm, wo_v)))]
    spans = ((0, 1), (1, 3), (3, 7), (7, 11), (11, n_pair))

    def row_loads(i):
        rows = slice(2 * spans[i][0], 2 * spans[i][1])
        return (load(kr_hbm.at[rows], kr_v.at[rows], kr_sem.at[i]), load(ckv_hbm.at[rows], ckv_v.at[rows], ckv_sem.at[i]))

    for w in (hid_load, *early):
        w.start()

    barrier = pltpu.get_barrier_semaphore()
    for peer in (sib, cnt, far):
        pl.semaphore_signal(barrier, inc=1, device_id={"seq": peer}, device_id_type=MESH)

    for i in range(len(spans)):
        for w in row_loads(i):
            w.start()
        if i == 2:
            for w in late:
                w.start()

    def remote(src, dst, send, recv, peer):
        return pltpu.make_async_remote_copy(
            src_ref=src, dst_ref=dst, send_sem=send, recv_sem=recv,
            device_id={"seq": peer}, device_id_type=MESH,
        )

    n_head = wqr_hbm.shape[0] // rope
    n_local = n_rows * n_head
    def row_of(r):
        j = (r // 4) % 2
        return 2 * (r // 8) + j + x - 2 * j * x

    r_h = iota((n_local, nope), 0) % 4
    same_head = iota((n_local, n_head * nope), 1) % n_head == iota((n_local, n_head * nope), 0) % 4
    spread = (iota((nope, n_head * nope), 1) // n_head == iota((nope, n_head * nope), 0)).astype(F32).astype(BF16)
    rep = (iota((n_local, n_rows), 1) == row_of(iota((n_local, n_rows), 0))).astype(F32).astype(BF16)
    fold = (iota((n_head * rope, STAT), 0) % rope == iota((n_head * rope, STAT), 1)).astype(F32).astype(BF16)
    hid_load.wait()
    hid_r[...] = dot(rep, hid_v[...]).astype(BF16)
    for k in range(d_model // nope):
        wide = dot(hid_r[:, k * nope:(k + 1) * nope], spread)
        em_v[:, k * n_head * nope:(k + 1) * n_head * nope] = jnp.where(same_head, wide, 0.0).astype(BF16)
    for w in early:
        w.wait()
    q_r = dot_t(hid_r[...], wqr_v[...])
    q_n = dot(em_v[...], wuq_v[...])
    q_r = jnp.where(iota((n_local, n_head * rope), 1) // rope == iota((n_local, n_head * rope), 0) % 4, q_r, 0.0)
    q_r = dot(q_r.astype(BF16), fold).astype(BF16)
    q_wide = jnp.concatenate([jnp.where(r_h == h, q_n, 0.0).astype(BF16) for h in range(n_head)], axis=1)
    q_l = dot(q_wide, wuk_v[...]).astype(BF16)
    for p in range(n_pair):
        qall[me, p, :, 0:lat] = q_l[8 * p:8 * p + 8]
        qall[me, p, :, lat:lat + STAT] = q_r[8 * p:8 * p + 8]

    pl.semaphore_wait(barrier, 3)

    chunks = ((0, 1), (1, 3), (3, 7), (7, 11), (11, n_pair))
    n_direct = 3

    def q_copy(kind, g):
        forward = g >= n_direct and kind == 1
        slot, peer = ((me, cnt), (cnt, sib) if forward else (me, far), (me, sib))[kind]
        rows = qall.at[slot, chunks[g][0]:chunks[g][1]]
        return remote(rows, rows, q_send, q_recv.at[g + 2 if g >= n_direct and kind == 0 else g], peer)

    def q_wait(g):
        rows = qall.at[0:2 if g >= n_direct else 3, chunks[g][0]:chunks[g][1]]
        remote(rows, rows, q_send, q_recv.at[g], sib).wait_recv()

    def q_forward(g):
        q_copy(0, g).wait_recv()
        q_copy(1, g).start()

    for g in range(n_direct):
        for kind in range(3):
            q_copy(kind, g).start()

    upper8 = iota((8, lat + STAT), 0) < 4

    def scores(p):
        tiles = [qall[s, p].astype(F32) for s in range(4)]
        q_even = jnp.concatenate([jnp.where(upper8, tiles[0], tiles[2]), jnp.where(upper8, tiles[1], tiles[3])], axis=0)
        q_odd = jnp.concatenate([jnp.where(upper8, tiles[2], tiles[0]), jnp.where(upper8, tiles[3], tiles[1])], axis=0)
        for i, q in enumerate((q_even, q_odd)):
            q = q.astype(BF16)
            b = 2 * p + i
            s = dot_t(q[:, :lat], ckv_v[b]) + dot(q[:, lat:lat + rope], kr_v[b])
            sbuf[p % 2, i] = s

    def wait_rows(p):
        for i, span in enumerate(spans):
            if p == span[0]:
                for w in row_loads(i):
                    w.wait()

    stat_lane = iota((16, STAT), 1) < STAT // 2

    def attend(p):
        for i in (0, 1):
            b = 2 * p + i
            s = sbuf[p % 2, i] * scale
            pos = me * shard + iota(s.shape, 1)
            s = jnp.where(pos < len_s[b], s, -jnp.inf)
            m = jnp.max(s, axis=1, keepdims=True)
            e = jnp.exp(s - jnp.where(m > -jnp.inf, m, 0.0))
            l = jnp.sum(e, axis=1, keepdims=True)
            acc = dot(e.astype(BF16), ckv_v[b])
            stat = jnp.where(stat_lane, m, l)
            for k in (0, 1):
                acc_src[k, b, :, 0:lat] = acc[8 * k:8 * k + 8]
                acc_src[k, b, :, lat:lat + STAT] = stat[8 * k:8 * k + 8]

    groups = ((0, 4), (4, 8), (8, 12), (12, 14), (14, n_pair))
    n_full = 3
    sends = ((0, 1), (2, 3), (4, 5), (6, 7), (8, 9), (10, 11), (12,), (13,), (14,), (15,))

    def pair_copy(ps):
        rows = slice(2 * ps[0], 2 * ps[-1] + 2)
        return remote(acc_src.at[1 - c, rows], r1.at[rows], a_send, a_recv.at[sends.index(ps)], sib)

    def chip_copy(ps):
        rows = slice(ps[0], ps[-1] + 1)
        g = max(i for i, group in enumerate(groups) if group[0] <= ps[0])
        return remote(s2.at[rows], r2.at[rows], c_send, c_recv.at[g], cnt)

    def chip_wait(g):
        rows = r2.at[groups[g][0]:groups[g][1]]
        remote(rows, rows, c_send, c_recv.at[g], cnt).wait_recv()

    def merge(a, b):
        m1, l1 = a[:, lat:lat + 1], a[:, lat + STAT // 2:lat + STAT // 2 + 1]
        m2, l2 = b[:, lat:lat + 1], b[:, lat + STAT // 2:lat + STAT // 2 + 1]
        m = jnp.maximum(m1, m2)
        shift = jnp.where(m > -jnp.inf, m, 0.0)
        w1, w2 = jnp.exp(m1 - shift), jnp.exp(m2 - shift)
        return w1 * a[:, :lat] + w2 * b[:, :lat], m, w1 * l1 + w2 * l2

    stat_lane8 = iota((8, STAT), 1) < STAT // 2

    def merge_pair(p):
        both = []
        for i in (0, 1):
            acc, m, l = merge(acc_src[c, 2 * p + i], r1[2 * p + i])
            both.append((acc, jnp.where(stat_lane8, m, l)))
        for k, (lo, hi) in enumerate(((0, lat), (lat, lat + STAT))):
            upper = upper8[:, lo:hi]
            zero = jnp.where(upper, both[0][k], both[1][k])
            one = jnp.where(upper, both[1][k], both[0][k])
            keep_v[p, :, lo:hi] = jnp.where(x == 0, zero, one)
            s2[p, :, lo:hi] = jnp.where(x == 0, one, zero)

    def o_rows(p):
        acc, _, l = merge(keep_v[p], r2[p])
        return acc / l

    def project(first, last):
        n_out, n_b = 8 * (last - first), 2 * (last - first)
        o_lat = jnp.concatenate([o_rows(p) for p in range(first, last)], axis=0).astype(BF16)
        head = iota((n_out, nope), 0) % 4
        wide = []
        for h in range(0, n_head, 2):
            two = dot(o_lat, jnp.concatenate([wuv_v[h], wuv_v[h + 1]], axis=1))
            wide += [jnp.where(head == h + i, two[:, i * nope:(i + 1) * nope], 0.0).astype(BF16) for i in (0, 1)]
        wide = jnp.concatenate(wide, axis=1)
        r = iota((n_b, n_out), 1)
        gather = (iota((n_b, n_out), 0) == row_of(r)).astype(F32).astype(BF16)
        o_val = dot(gather, wide).astype(BF16)
        return lambda k: dot(o_val, wo_v[:, pl.ds(pl.multiple_of(k * half_d, half_d), half_d)])

    def project_full(g, n=1):
        y = project(groups[g][0], groups[g + n - 1][1])
        for k in (0, 1):
            part = y(k)
            for i in range(n):
                y_src[g + i, k] = part[8 * i:8 * i + 8]

    def project_last(g):
        y = project(*groups[g])
        i = g - n_full
        l_src[i, 1 - c] = y(1 - c)
        remote(l_src.at[i, 1 - c], l_r1.at[i], l_send.at[0], l_recv.at[0, i], sib).start()
        l_src[i, c] = y(c)

    def y_copy(kind, g):
        if kind == 0:
            return remote(y_src.at[g, 1 - c], yr1.at[g], y_send, y_recv.at[0, g], sib)
        return remote(yc.at[g], yr2.at[g], y_send, y_recv.at[1, g], cnt)

    def f_copy(g):
        return remote(f_src.at[g], f_rcv.at[g], f_send, f_recv, sib)

    def last_chip(g):
        i = g - n_full
        remote(l_r1.at[i], l_r1.at[i], l_send.at[0], l_recv.at[0, i], sib).wait_recv()
        l_sum[i] = l_src[i, c] + l_r1[i]
        for k, peer in enumerate((cnt, far, sib)):
            remote(l_sum.at[i], l_all.at[i, k], l_send.at[1], l_recv.at[1, i], peer).start()

    def last_final(g):
        i = g - n_full
        remote(l_all.at[i], l_all.at[i], l_send.at[1], l_recv.at[1, i], sib).wait_recv()
        rows = slice(2 * groups[g][0] % 8, (2 * groups[g][1] - 1) % 8 + 1)
        put(2 * groups[g][0] // 8, rows, l_sum[i] + l_all[i, 0], l_all[i, 2] + l_all[i, 1])

    def y_chip(g):
        y_copy(0, g).wait_recv()
        yc[g] = y_src[g, c] + yr1[g]
        y_copy(1, g).start()

    def hid_half(g, k, rows=slice(None)):
        return hid3_v[g, rows, pl.ds(pl.multiple_of(k * half_d, half_d), half_d)].astype(F32)

    def y_final(g):
        y_copy(1, g).wait_recv()
        f_src[g] = (hid_half(g, c) + (yc[g] + yr2[g])).astype(BF16)
        f_copy(g).start()

    def put(g, rows, mine, other):
        hid = hid3_v[g, rows, :].astype(F32)
        out_ref[g, rows, 0:half_d] = (hid[:, :half_d] + jnp.where(c == 0, mine, other)).astype(BF16)
        out_ref[g, rows, half_d:d_model] = (hid[:, half_d:] + jnp.where(c == 0, other, mine)).astype(BF16)

    def step(js, merges=(), ready=()):
        for j in js:
            wait_rows(j)
        if merges:
            pair_copy(merges).wait_recv()
        for g in ready:
            chip_wait(g)
        for j in js:
            scores(j)
            attend(j - 1)
        for p in merges:
            merge_pair(p)
        for g in ready:
            project_full(g)
        pair_copy(tuple(j - 1 for j in js)).start()
        if merges:
            chip_copy(merges).start()
        for g in ready:
            y_copy(0, g).start()

    q_wait(0)
    for g in range(n_direct, len(chunks)):
        for kind in (0, 2):
            q_copy(kind, g).start()
    wait_rows(0)
    scores(0)
    q_wait(1)
    step((1, 2))
    q_wait(2)
    step((3, 4))
    q_forward(3)
    step((5, 6), (0, 1))
    q_forward(4)
    q_wait(3)
    step((7, 8), (2, 3))
    step((9, 10), (4, 5))
    q_wait(4)
    step((11, 12), (6, 7))
    for w in late:
        w.wait()
    step((13,), (8, 9))
    step((14,), (10, 11), (0,))
    step((15,), (12,))
    attend(n_pair - 1)
    pair_copy((n_pair - 1,)).start()

    def last_merge(ps):
        pair_copy(ps).wait_recv()
        for p in ps:
            merge_pair(p)
        chip_copy(ps).start()

    last_merge((13,))
    last_merge((14,))
    last_merge((15,))
    y_chip(0)
    chip_wait(1)
    chip_wait(2)
    project_full(1, 2)
    for g in (1, 2):
        y_copy(0, g).start()
    y_chip(1)
    y_chip(2)
    chip_wait(3)
    project_last(3)
    chip_wait(4)
    project_last(4)
    last_chip(3)
    last_chip(4)
    for g in range(n_full):
        y_final(g)
    remote(f_rcv, f_rcv, f_send, f_recv, sib).wait_recv()
    for g in range(n_full):
        mine, other = f_src[g].astype(F32), f_rcv[g].astype(F32)
        out_ref[g, :, 0:half_d] = jnp.where(c == 0, mine, other).astype(BF16)
        out_ref[g, :, half_d:d_model] = jnp.where(c == 0, other, mine).astype(BF16)
    last_final(3)
    remote(qall.at[0:3], qall.at[0:3], q_send, q_recv.at[0], sib).wait_send()
    remote(r1, r1, a_send, a_recv.at[0], sib).wait_send()
    remote(r2, r2, c_send, c_recv.at[0], cnt).wait_send()
    remote(f_rcv, f_rcv, f_send, f_recv, sib).wait_send()
    remote(y_src, y_src, y_send, y_recv.at[0, 0], sib).wait_send()
    remote(l_r1, l_r1, l_send.at[0], l_recv.at[0, 0], sib).wait_send()
    remote(l_all, l_all, l_send.at[1], l_recv.at[0, 0], sib).wait_send()
    last_final(4)


def solution(mesh):
    row_spec = P('batch', None)
    cache_spec = P('batch', 'seq', None)
    in_specs = (row_spec, P('batch'), cache_spec, cache_spec, P(None, 'seq', None), P(None, 'seq', None), P('seq', None, None), P('seq', None, None), P('seq', None, None))

    def mla_step(hidden, lengths, c_kv, k_rope, w_uq, w_qr, w_uk, w_uv, w_o):
        n_rows, d_model = hidden.shape
        _, shard, lat = c_kv.shape
        rope = k_rope.shape[2]
        n_head, nope = w_uq.shape[1], w_uq.shape[2]
        n_pair = n_rows // 2
        n_group = n_pair // GROUP
        wide = lat + STAT
        half = d_model // 2
        hid3 = hidden.reshape(n_group, 8, d_model)
        operands = (
            lengths,
            hidden,
            hid3,
            w_uq.reshape(d_model * n_head, nope),
            jnp.transpose(w_qr, (1, 2, 0)).reshape(n_head * rope, d_model),
            w_uk.reshape(n_head * nope, lat),
            w_uv,
            w_o.reshape(n_head * w_o.shape[1], d_model),
            c_kv,
            jnp.transpose(k_rope, (0, 2, 1)),
        )
        operands = tuple(pltpu.with_memory_space_constraint(a, pltpu.HBM) for a in operands)
        vm = pltpu.VMEM
        dma = pltpu.SemaphoreType.DMA
        out = pl.pallas_call(
            kernel,
            out_shape=jax.ShapeDtypeStruct((n_group, 8, d_model), BF16),
            in_specs=[pl.BlockSpec(memory_space=pltpu.HBM)] * len(operands),
            out_specs=pl.BlockSpec(memory_space=pltpu.VMEM),
            scratch_shapes=[
                pltpu.SMEM((n_rows,), jnp.int32),
                vm(hidden.shape, BF16),
                vm(hid3.shape, BF16),
                vm((n_head * n_rows, d_model), BF16),
                vm(operands[3].shape, BF16),
                vm(operands[4].shape, BF16),
                vm(operands[5].shape, BF16),
                vm(operands[6].shape, BF16),
                vm(operands[7].shape, BF16),
                vm(c_kv.shape, BF16),
                vm(operands[9].shape, BF16),
                vm((n_head * n_rows, n_head * d_model), BF16),
                vm((4, n_pair, 8, wide), BF16),
                vm((2, 2, 16, shard), F32),
                vm((2, n_rows, 8, wide), F32),
                vm((n_rows, 8, wide), F32),
                vm((n_pair, 8, wide), F32),
                vm((n_pair, 8, wide), F32),
                vm((n_pair, 8, wide), F32),
                vm((3, 2, 8, half), F32),
                vm((3, 8, half), F32),
                vm((3, 8, half), F32),
                vm((3, 8, half), F32),
                vm((3, 8, half), BF16),
                vm((3, 8, half), BF16),
                vm((2, 2, 4, half), F32),
                vm((2, 4, half), F32),
                vm((2, 4, half), F32),
                vm((2, 3, 4, half), F32),
                dma((8,)),
                dma((5,)),
                dma((5,)),
                dma(()),
                dma((7,)),
                dma(()),
                dma((10,)),
                dma(()),
                dma((5,)),
                dma(()),
                dma((2, 3)),
                dma(()),
                dma(()),
                dma((2,)),
                dma((2, 2)),
            ],
            compiler_params=pltpu.CompilerParams(
                collective_id=0, has_side_effects=True, vmem_limit_bytes=53 * 1024 * 1024,
            ),
            name="mla_decode",
        )(*operands)
        return out.reshape(n_rows, d_model)

    return jax.shard_map(mla_step, mesh=mesh, in_specs=in_specs, out_specs=row_spec, check_vma=False)
```

```python
import math

import jax
import jax.numpy as jnp
from jax import lax
from jax.experimental import pallas as pl
from jax.experimental.pallas import tpu as pltpu
from jax.sharding import PartitionSpec as P

MESH = pl.DeviceIdType.MESH
F32 = jnp.float32
BF16 = jnp.bfloat16
GROUP = 4
STAT = 128


def dot(a, b):
    return jnp.dot(a, b, preferred_element_type=F32)


def dot_t(a, b):
    return lax.dot_general(a, b, (((1,), (1,)), ((), ())), preferred_element_type=F32)


def iota(shape, dim):
    return lax.broadcasted_iota(jnp.int32, shape, dim)


def kernel(
    len_hbm, hid_hbm, hid3_hbm, wuq_hbm, wqr_hbm, wuk_hbm, wuv_hbm, wo_hbm, ckv_hbm, kr_hbm,
    out_ref,
    len_s, hid_v, hid3_v, hid_r, wuq_v, wqr_v, wuk_v, wuv_v, wo_v, ckv_v, kr_v,
    em_v, qall, sbuf, acc_src, r1, s2, keep_v, r2, y_src, yr1, yc, yr2, f_src, f_rcv, h_src, h_rcv, l_src, l_r1, l_sum, l_all,
    w_sem, ckv_sem, sent, q_recv, a_recv, c_recv, y_recv, f_recv, h_recv, l_recv,
):
    n_rows = ckv_hbm.shape[0]
    shard = ckv_hbm.shape[1]
    lat = ckv_hbm.shape[2]
    rope = kr_hbm.shape[1]
    nope = wuq_hbm.shape[1]
    n_pair = n_rows // 2
    d_model = hid_hbm.shape[1]
    half_d = d_model // 2
    scale = 1.0 / math.sqrt(nope + rope)

    me = lax.axis_index("seq")
    x = lax.div(me, 2)
    c = lax.rem(me, 2)
    sib = 2 * x + (1 - c)
    cnt = 2 * (1 - x) + c
    far = 3 - me

    def load(src, dst, sem):
        return pltpu.make_async_copy(src, dst, sem)

    hid_load = load(hid_hbm, hid_v, w_sem.at[0])
    early = [load(src, dst, w_sem.at[min(1 + i, 3)]) for i, (src, dst) in enumerate((
        (wqr_hbm, wqr_v), (wuq_hbm, wuq_v), (wuk_hbm, wuk_v), (len_hbm, len_s), (hid3_hbm, hid3_v)))]
    late = [load(src, dst, w_sem.at[4]) for src, dst in ((wuv_hbm, wuv_v), (wo_hbm, wo_v))]
    spans = ((0, 1), (1, 3), (3, 7), (7, 11), (11, n_pair))

    def row_loads(i):
        rows = slice(2 * spans[i][0], 2 * spans[i][1])
        return (load(kr_hbm.at[rows], kr_v.at[rows], ckv_sem.at[i]), load(ckv_hbm.at[rows], ckv_v.at[rows], ckv_sem.at[i]))

    for w in (hid_load, *early):
        w.start()

    barrier = pltpu.get_barrier_semaphore()
    for peer in (sib, cnt, far):
        pl.semaphore_signal(barrier, inc=1, device_id={"seq": peer}, device_id_type=MESH)

    for i in range(len(spans)):
        for w in row_loads(i):
            w.start()
        if i == 2:
            for w in late:
                w.start()

    def remote(src, dst, send, recv, peer):
        return pltpu.make_async_remote_copy(
            src_ref=src, dst_ref=dst, send_sem=send, recv_sem=recv,
            device_id={"seq": peer}, device_id_type=MESH,
        )

    n_head = wqr_hbm.shape[0] // rope
    n_local = n_rows * n_head
    def row_of(r):
        j = (r // 4) % 2
        return 2 * (r // 8) + j + x - 2 * j * x

    r_h = iota((n_local, nope), 0) % 4
    same_head = iota((n_local, n_head * nope), 1) % n_head == iota((n_local, n_head * nope), 0) % 4
    spread = (iota((nope, n_head * nope), 1) // n_head == iota((nope, n_head * nope), 0)).astype(F32).astype(BF16)
    rep = (iota((n_local, n_rows), 1) == row_of(iota((n_local, n_rows), 0))).astype(F32).astype(BF16)
    fold = (iota((n_head * rope, STAT), 0) % rope == iota((n_head * rope, STAT), 1)).astype(F32).astype(BF16)
    hid_load.wait()
    hid_r[...] = dot(rep, hid_v[...]).astype(BF16)
    for k in range(d_model // nope):
        wide = dot(hid_r[:, k * nope:(k + 1) * nope], spread)
        em_v[:, k * n_head * nope:(k + 1) * n_head * nope] = jnp.where(same_head, wide, 0.0).astype(BF16)
    for w in early[:2]:
        w.wait()
    q_r = dot_t(hid_r[...], wqr_v[...])
    q_n = dot(em_v[...], wuq_v[...])
    q_r = jnp.where(iota((n_local, n_head * rope), 1) // rope == iota((n_local, n_head * rope), 0) % 4, q_r, 0.0)
    q_r = dot(q_r.astype(BF16), fold).astype(BF16)
    q_wide = jnp.concatenate([jnp.where(r_h == h, q_n, 0.0).astype(BF16) for h in range(n_head)], axis=1)
    for w in early[2:]:
        w.wait()
    q_l = dot(q_wide, wuk_v[...]).astype(BF16)
    for p in range(n_pair):
        qall[me, p, :, 0:lat] = q_l[8 * p:8 * p + 8]
        qall[me, p, :, lat:lat + STAT] = q_r[8 * p:8 * p + 8]

    pl.semaphore_wait(barrier, 3)

    chunks = ((0, 1), (1, 3), (3, 7), (7, 11), (11, n_pair))
    n_direct = 3

    def q_copy(kind, g):
        forward = g >= n_direct and kind == 1
        slot, peer = ((me, cnt), (cnt, sib) if forward else (me, far), (me, sib))[kind]
        rows = qall.at[slot, chunks[g][0]:chunks[g][1]]
        return remote(rows, rows, sent, q_recv.at[g + 2 if g >= n_direct and kind == 0 else g], peer)

    def q_wait(g):
        rows = qall.at[0:2 if g >= n_direct else 3, chunks[g][0]:chunks[g][1]]
        remote(rows, rows, sent, q_recv.at[g], sib).wait_recv()

    def q_forward(g):
        q_copy(0, g).wait_recv()
        q_copy(1, g).start()

    for g in range(n_direct):
        for kind in range(3):
            q_copy(kind, g).start()

    upper8 = iota((8, lat + STAT), 0) < 4

    def scores(p):
        tiles = [qall[s, p].astype(F32) for s in range(4)]
        q_even = jnp.concatenate([jnp.where(upper8, tiles[0], tiles[2]), jnp.where(upper8, tiles[1], tiles[3])], axis=0)
        q_odd = jnp.concatenate([jnp.where(upper8, tiles[2], tiles[0]), jnp.where(upper8, tiles[3], tiles[1])], axis=0)
        for i, q in enumerate((q_even, q_odd)):
            q = q.astype(BF16)
            b = 2 * p + i
            s = dot_t(q[:, :lat], ckv_v[b]) + dot(q[:, lat:lat + rope], kr_v[b])
            sbuf[p % 2, i] = s

    def wait_rows(p):
        for i, span in enumerate(spans):
            if p == span[0]:
                for w in row_loads(i):
                    w.wait()

    stat_lane = iota((16, STAT), 1) < STAT // 2

    def attend(p):
        for i in (0, 1):
            b = 2 * p + i
            s = sbuf[p % 2, i] * scale
            pos = me * shard + iota(s.shape, 1)
            s = jnp.where(pos < len_s[b], s, -jnp.inf)
            m = jnp.max(s, axis=1, keepdims=True)
            e = jnp.exp(s - jnp.where(m > -jnp.inf, m, 0.0))
            l = jnp.sum(e, axis=1, keepdims=True)
            acc = dot(e.astype(BF16), ckv_v[b])
            stat = jnp.where(stat_lane, m, l)
            for k in (0, 1):
                acc_src[k, b, :, 0:lat] = acc[8 * k:8 * k + 8]
                acc_src[k, b, :, lat:lat + STAT] = stat[8 * k:8 * k + 8]

    groups = ((0, 4), (4, 8), (8, 12), (12, 14), (14, n_pair))
    n_full = 3
    sends = ((0, 1), (2, 3), (4, 5), (6, 7), (8, 9), (10, 11), (12,), (13,), (14,), (15,))

    def pair_copy(ps):
        rows = slice(2 * ps[0], 2 * ps[-1] + 2)
        return remote(acc_src.at[1 - c, rows], r1.at[rows], sent, a_recv.at[sends.index(ps)], sib)

    def chip_copy(ps):
        rows = slice(ps[0], ps[-1] + 1)
        g = max(i for i, group in enumerate(groups) if group[0] <= ps[0])
        return remote(s2.at[rows], r2.at[rows], sent, c_recv.at[g], cnt)

    def chip_wait(g):
        rows = r2.at[groups[g][0]:groups[g][1]]
        remote(rows, rows, sent, c_recv.at[g], cnt).wait_recv()

    def merge(a, b):
        m1, l1 = a[:, lat:lat + 1], a[:, lat + STAT // 2:lat + STAT // 2 + 1]
        m2, l2 = b[:, lat:lat + 1], b[:, lat + STAT // 2:lat + STAT // 2 + 1]
        m = jnp.maximum(m1, m2)
        shift = jnp.where(m > -jnp.inf, m, 0.0)
        w1, w2 = jnp.exp(m1 - shift), jnp.exp(m2 - shift)
        return w1 * a[:, :lat] + w2 * b[:, :lat], m, w1 * l1 + w2 * l2

    stat_lane8 = iota((8, STAT), 1) < STAT // 2

    def merge_pair(p):
        both = []
        for i in (0, 1):
            acc, m, l = merge(acc_src[c, 2 * p + i], r1[2 * p + i])
            both.append((acc, jnp.where(stat_lane8, m, l)))
        for k, (lo, hi) in enumerate(((0, lat), (lat, lat + STAT))):
            upper = upper8[:, lo:hi]
            zero = jnp.where(upper, both[0][k], both[1][k])
            one = jnp.where(upper, both[1][k], both[0][k])
            keep_v[p, :, lo:hi] = jnp.where(x == 0, zero, one)
            s2[p, :, lo:hi] = jnp.where(x == 0, one, zero)

    def o_rows(p):
        acc, _, l = merge(keep_v[p], r2[p])
        return acc / l

    def project(first, last):
        n_out, n_b = 8 * (last - first), 2 * (last - first)
        o_lat = jnp.concatenate([o_rows(p) for p in range(first, last)], axis=0).astype(BF16)
        head = iota((n_out, nope), 0) % 4
        wide = []
        for h in range(0, n_head, 2):
            two = dot(o_lat, jnp.concatenate([wuv_v[h], wuv_v[h + 1]], axis=1))
            wide += [jnp.where(head == h + i, two[:, i * nope:(i + 1) * nope], 0.0).astype(BF16) for i in (0, 1)]
        wide = jnp.concatenate(wide, axis=1)
        r = iota((n_b, n_out), 1)
        gather = (iota((n_b, n_out), 0) == row_of(r)).astype(F32).astype(BF16)
        o_val = dot(gather, wide).astype(BF16)
        return lambda k: dot(o_val, wo_v[:, pl.ds(pl.multiple_of(k * half_d, half_d), half_d)])

    def project_full(g):
        y = project(*groups[g])
        for k in (0, 1):
            y_src[g, k] = y(k)

    def project_last(g):
        y = project(*groups[g])
        i = g - n_full
        l_src[i, 1 - c] = y(1 - c)
        remote(l_src.at[i, 1 - c], l_r1.at[i], sent, l_recv.at[0, i], sib).start()
        l_src[i, c] = y(c)

    def y_copy(kind, g):
        if kind == 0:
            return remote(y_src.at[g, 1 - c], yr1.at[g], sent, y_recv.at[0, g], sib)
        return remote(yc.at[g], yr2.at[g], sent, y_recv.at[1, g], cnt)

    def f_copy(g):
        return remote(f_src.at[g], f_rcv.at[g], sent, f_recv, sib)

    def last_chip(g):
        i = g - n_full
        remote(l_r1.at[i], l_r1.at[i], sent, l_recv.at[0, i], sib).wait_recv()
        l_sum[i] = l_src[i, c] + l_r1[i]
        for k, peer in enumerate((cnt, far, sib)[:1 + 2 * i]):
            remote(l_sum.at[i], l_all.at[i, k], sent, l_recv.at[1, i], peer).start()

    def rows_of(g):
        return slice(2 * groups[g][0] % 8, (2 * groups[g][1] - 1) % 8 + 1)

    def half_copy():
        return remote(h_src, h_rcv, sent, h_recv, sib)

    def half_final(g):
        i = g - n_full
        remote(l_all.at[i, 0], l_all.at[i, 0], sent, l_recv.at[1, i], sib).wait_recv()
        h_src[...] = (hid_half(2 * groups[g][0] // 8, c, rows_of(g)) + (l_sum[i] + l_all[i, 0])).astype(BF16)
        half_copy().start()

    def last_final(g):
        i = g - n_full
        remote(l_all.at[i], l_all.at[i], sent, l_recv.at[1, i], sib).wait_recv()
        put(2 * groups[g][0] // 8, rows_of(g), l_sum[i] + l_all[i, 0], l_all[i, 2] + l_all[i, 1])

    def join(g, rows, mine, other):
        mine, other = mine.astype(F32), other.astype(F32)
        out_ref[g, rows, 0:half_d] = jnp.where(c == 0, mine, other).astype(BF16)
        out_ref[g, rows, half_d:d_model] = jnp.where(c == 0, other, mine).astype(BF16)

    def y_chip(g):
        y_copy(0, g).wait_recv()
        yc[g] = y_src[g, c] + yr1[g]
        y_copy(1, g).start()

    def hid_half(g, k, rows=slice(None)):
        return hid3_v[g, rows, pl.ds(pl.multiple_of(k * half_d, half_d), half_d)].astype(F32)

    def y_final(g):
        y_copy(1, g).wait_recv()
        f_src[g] = (hid_half(g, c) + (yc[g] + yr2[g])).astype(BF16)
        f_copy(g).start()

    def put(g, rows, mine, other):
        hid = hid3_v[g, rows, :].astype(F32)
        out_ref[g, rows, 0:half_d] = (hid[:, :half_d] + jnp.where(c == 0, mine, other)).astype(BF16)
        out_ref[g, rows, half_d:d_model] = (hid[:, half_d:] + jnp.where(c == 0, other, mine)).astype(BF16)

    def step(js, merges=(), ready=()):
        for j in js:
            wait_rows(j)
        if merges:
            pair_copy(merges).wait_recv()
        for g in ready:
            chip_wait(g)
        for j in js:
            scores(j)
            attend(j - 1)
        for p in merges:
            merge_pair(p)
        for g in ready:
            project_full(g)
        pair_copy(tuple(j - 1 for j in js)).start()
        if merges:
            chip_copy(merges).start()
        for g in ready:
            y_copy(0, g).start()

    q_wait(0)
    for g in range(n_direct, len(chunks)):
        for kind in (0, 2):
            q_copy(kind, g).start()
    wait_rows(0)
    scores(0)
    q_wait(1)
    step((1, 2))
    q_wait(2)
    step((3, 4))
    q_forward(3)
    step((5, 6), (0, 1))
    q_forward(4)
    q_wait(3)
    step((7, 8), (2, 3))
    step((9, 10), (4, 5))
    q_wait(4)
    step((11, 12), (6, 7))
    for w in late:
        w.wait()
    step((13,), (8, 9), (0,))
    step((14,), (10, 11))
    step((15,), (12,))
    attend(n_pair - 1)
    pair_copy((n_pair - 1,)).start()

    def last_merge(ps):
        pair_copy(ps).wait_recv()
        for p in ps:
            merge_pair(p)
        chip_copy(ps).start()

    last_merge((13,))
    last_merge((14,))
    last_merge((15,))
    for g in (1, 2):
        chip_wait(g)
        project_full(g)
        y_copy(0, g).start()
    y_chip(0)
    y_chip(1)
    chip_wait(3)
    project_last(3)
    y_chip(2)
    chip_wait(4)
    project_last(4)
    last_chip(3)
    last_chip(4)
    for g in range(n_full):
        y_final(g)
    half_final(3)
    remote(f_rcv, f_rcv, sent, f_recv, sib).wait_recv()
    for g in range(n_full):
        join(g, slice(None), f_src[g], f_rcv[g])
    half_copy().wait_recv()
    join(2 * groups[3][0] // 8, rows_of(3), h_src[...], h_rcv[...])
    half_copy().wait_send()
    remote(qall.at[0:3], qall.at[0:3], sent, q_recv.at[0], sib).wait_send()
    remote(r1, r1, sent, a_recv.at[0], sib).wait_send()
    remote(r2, r2, sent, c_recv.at[0], cnt).wait_send()
    remote(f_rcv, f_rcv, sent, f_recv, sib).wait_send()
    remote(y_src, y_src, sent, y_recv.at[0, 0], sib).wait_send()
    remote(l_r1, l_r1, sent, l_recv.at[0, 0], sib).wait_send()
    remote(l_src, l_src, sent, l_recv.at[0, 0], sib).wait_send()
    last_final(4)


def solution(mesh):
    row_spec = P('batch', None)
    cache_spec = P('batch', 'seq', None)
    in_specs = (row_spec, P('batch'), cache_spec, cache_spec, P(None, 'seq', None), P(None, 'seq', None), P('seq', None, None), P('seq', None, None), P('seq', None, None))

    def mla_step(hidden, lengths, c_kv, k_rope, w_uq, w_qr, w_uk, w_uv, w_o):
        n_rows, d_model = hidden.shape
        _, shard, lat = c_kv.shape
        rope = k_rope.shape[2]
        n_head, nope = w_uq.shape[1], w_uq.shape[2]
        n_pair = n_rows // 2
        n_group = n_pair // GROUP
        wide = lat + STAT
        half = d_model // 2
        hid3 = hidden.reshape(n_group, 8, d_model)
        operands = (
            lengths,
            hidden,
            hid3,
            w_uq.reshape(d_model * n_head, nope),
            jnp.transpose(w_qr, (1, 2, 0)).reshape(n_head * rope, d_model),
            w_uk.reshape(n_head * nope, lat),
            w_uv,
            w_o.reshape(n_head * w_o.shape[1], d_model),
            c_kv,
            jnp.transpose(k_rope, (0, 2, 1)),
        )
        operands = tuple(pltpu.with_memory_space_constraint(a, pltpu.HBM) for a in operands)
        vm = pltpu.VMEM
        dma = pltpu.SemaphoreType.DMA
        out = pl.pallas_call(
            kernel,
            out_shape=jax.ShapeDtypeStruct((n_group, 8, d_model), BF16),
            in_specs=[pl.BlockSpec(memory_space=pltpu.HBM)] * len(operands),
            out_specs=pl.BlockSpec(memory_space=pltpu.VMEM),
            scratch_shapes=[
                pltpu.SMEM((n_rows,), jnp.int32),
                vm(hidden.shape, BF16),
                vm(hid3.shape, BF16),
                vm((n_head * n_rows, d_model), BF16),
                vm(operands[3].shape, BF16),
                vm(operands[4].shape, BF16),
                vm(operands[5].shape, BF16),
                vm(operands[6].shape, BF16),
                vm(operands[7].shape, BF16),
                vm(c_kv.shape, BF16),
                vm(operands[9].shape, BF16),
                vm((n_head * n_rows, n_head * d_model), BF16),
                vm((4, n_pair, 8, wide), BF16),
                vm((2, 2, 16, shard), F32),
                vm((2, n_rows, 8, wide), F32),
                vm((n_rows, 8, wide), F32),
                vm((n_pair, 8, wide), F32),
                vm((n_pair, 8, wide), F32),
                vm((n_pair, 8, wide), F32),
                vm((3, 2, 8, half), F32),
                vm((3, 8, half), F32),
                vm((3, 8, half), F32),
                vm((3, 8, half), F32),
                vm((3, 8, half), BF16),
                vm((3, 8, half), BF16),
                vm((4, half), BF16),
                vm((4, half), BF16),
                vm((2, 2, 4, half), F32),
                vm((2, 4, half), F32),
                vm((2, 4, half), F32),
                vm((2, 3, 4, half), F32),
                dma((5,)),
                dma((5,)),
                dma(()),
                dma((7,)),
                dma((10,)),
                dma((5,)),
                dma((2, 3)),
                dma(()),
                dma(()),
                dma((2, 2)),
            ],
            compiler_params=pltpu.CompilerParams(
                collective_id=0, has_side_effects=True, vmem_limit_bytes=53 * 1024 * 1024,
            ),
            name="mla_decode",
        )(*operands)
        return out.reshape(n_rows, d_model)

    return jax.shard_map(mla_step, mesh=mesh, in_specs=in_specs, out_specs=row_spec, check_vma=False)
```

```python
import math

import jax
import jax.numpy as jnp
from jax import lax
from jax.experimental import pallas as pl
from jax.experimental.pallas import tpu as pltpu
from jax.sharding import PartitionSpec as P

MESH = pl.DeviceIdType.MESH
F32 = jnp.float32
BF16 = jnp.bfloat16
GROUP = 4
STAT = 128


def dot(a, b):
    return jnp.dot(a, b, preferred_element_type=F32)


def dot_t(a, b):
    return lax.dot_general(a, b, (((1,), (1,)), ((), ())), preferred_element_type=F32)


def iota(shape, dim):
    return lax.broadcasted_iota(jnp.int32, shape, dim)


def kernel(
    len_hbm, hid_hbm, hid3_hbm, wuq_hbm, wqr_hbm, wuk_hbm, wuv_hbm, wo_hbm, ckv_hbm, kr_hbm,
    out_ref,
    len_s, hid_v, hid3_v, hid_r, wuq_v, wqr_v, wuk_v, wuv_v, wo_v, ckv_v, kr_v,
    em_v, qall, sbuf, acc_src, r1, s2, keep_v, r2, y_src, yr1, yc, yr2, f_src, f_rcv, h_src, h_rcv, l_src, l_r1, l_sum, l_all,
    w_sem, ckv_sem, sent, q_recv, a_recv, c_recv,
):
    n_rows = ckv_hbm.shape[0]
    shard = ckv_hbm.shape[1]
    lat = ckv_hbm.shape[2]
    rope = kr_hbm.shape[1]
    nope = wuq_hbm.shape[1]
    n_pair = n_rows // 2
    d_model = hid_hbm.shape[1]
    half_d = d_model // 2
    scale = 1.0 / math.sqrt(nope + rope)

    me = lax.axis_index("seq")
    x = lax.div(me, 2)
    c = lax.rem(me, 2)
    sib = 2 * x + (1 - c)
    cnt = 2 * (1 - x) + c
    far = 3 - me

    def load(src, dst, sem):
        return pltpu.make_async_copy(src, dst, sem)

    hid_load = load(hid_hbm, hid_v, w_sem.at[0])
    early = [load(src, dst, w_sem.at[min(1 + i, 3)]) for i, (src, dst) in enumerate((
        (wqr_hbm, wqr_v), (wuq_hbm, wuq_v), (wuk_hbm, wuk_v), (len_hbm, len_s), (hid3_hbm, hid3_v)))]
    late = [load(src, dst, w_sem.at[4]) for src, dst in ((wuv_hbm, wuv_v), (wo_hbm, wo_v))]
    spans = ((0, 1), (1, 3), (3, 7), (7, 11), (11, n_pair))

    def row_loads(i):
        rows = slice(2 * spans[i][0], 2 * spans[i][1])
        return (load(kr_hbm.at[rows], kr_v.at[rows], ckv_sem.at[i]), load(ckv_hbm.at[rows], ckv_v.at[rows], ckv_sem.at[i]))

    for w in (hid_load, *early):
        w.start()

    barrier = pltpu.get_barrier_semaphore()
    for peer in (sib, cnt, far):
        pl.semaphore_signal(barrier, inc=1, device_id={"seq": peer}, device_id_type=MESH)

    for i in range(len(spans)):
        for w in row_loads(i):
            w.start()
        if i == 2:
            for w in late:
                w.start()

    def remote(src, dst, send, recv, peer):
        return pltpu.make_async_remote_copy(
            src_ref=src, dst_ref=dst, send_sem=send, recv_sem=recv,
            device_id={"seq": peer}, device_id_type=MESH,
        )

    n_head = wqr_hbm.shape[0] // rope
    n_local = n_rows * n_head
    def row_of(r):
        j = (r // 4) % 2
        return 2 * (r // 8) + j + x - 2 * j * x

    r_h = iota((n_local, nope), 0) % 4
    same_head = iota((n_local, n_head * nope), 1) % n_head == iota((n_local, n_head * nope), 0) % 4
    spread = (iota((nope, n_head * nope), 1) // n_head == iota((nope, n_head * nope), 0)).astype(F32).astype(BF16)
    rep = (iota((n_local, n_rows), 1) == row_of(iota((n_local, n_rows), 0))).astype(F32).astype(BF16)
    fold = (iota((n_head * rope, STAT), 0) % rope == iota((n_head * rope, STAT), 1)).astype(F32).astype(BF16)
    hid_load.wait()
    hid_r[...] = dot(rep, hid_v[...]).astype(BF16)
    for k in range(d_model // nope):
        wide = dot(hid_r[:, k * nope:(k + 1) * nope], spread)
        em_v[:, k * n_head * nope:(k + 1) * n_head * nope] = jnp.where(same_head, wide, 0.0).astype(BF16)
    for w in early[:2]:
        w.wait()
    q_r = dot_t(hid_r[...], wqr_v[...])
    q_n = dot(em_v[...], wuq_v[...])
    q_r = jnp.where(iota((n_local, n_head * rope), 1) // rope == iota((n_local, n_head * rope), 0) % 4, q_r, 0.0)
    q_r = dot(q_r.astype(BF16), fold).astype(BF16)
    q_wide = jnp.concatenate([jnp.where(r_h == h, q_n, 0.0).astype(BF16) for h in range(n_head)], axis=1)
    for w in early[2:]:
        w.wait()
    q_l = dot(q_wide, wuk_v[...]).astype(BF16)
    for p in range(n_pair):
        qall[me, p, :, 0:lat] = q_l[8 * p:8 * p + 8]
        qall[me, p, :, lat:lat + STAT] = q_r[8 * p:8 * p + 8]

    pl.semaphore_wait(barrier, 3)

    chunks = ((0, 1), (1, 3), (3, 7), (7, 11), (11, n_pair))
    n_direct = 3

    def q_copy(kind, g):
        forward = g >= n_direct and kind == 1
        slot, peer = ((me, cnt), (cnt, sib) if forward else (me, far), (me, sib))[kind]
        rows = qall.at[slot, chunks[g][0]:chunks[g][1]]
        return remote(rows, rows, sent, q_recv.at[g + 2 if g >= n_direct and kind == 0 else g], peer)

    def q_wait(g):
        rows = qall.at[0:2 if g >= n_direct else 3, chunks[g][0]:chunks[g][1]]
        remote(rows, rows, sent, q_recv.at[g], sib).wait_recv()

    def q_forward(g):
        q_copy(0, g).wait_recv()
        q_copy(1, g).start()

    for g in range(n_direct):
        for kind in range(3):
            q_copy(kind, g).start()


    upper8 = iota((8, lat + STAT), 0) < 4

    def scores(p):
        tiles = [qall[s, p].astype(F32) for s in range(4)]
        q_even = jnp.concatenate([jnp.where(upper8, tiles[0], tiles[2]), jnp.where(upper8, tiles[1], tiles[3])], axis=0)
        q_odd = jnp.concatenate([jnp.where(upper8, tiles[2], tiles[0]), jnp.where(upper8, tiles[3], tiles[1])], axis=0)
        for i, q in enumerate((q_even, q_odd)):
            q = q.astype(BF16)
            b = 2 * p + i
            s = dot_t(q[:, :lat], ckv_v[b]) + dot(q[:, lat:lat + rope], kr_v[b])
            sbuf[p % 2, i] = s

    def wait_rows(p):
        for i, span in enumerate(spans):
            if p == span[0]:
                for w in row_loads(i):
                    w.wait()

    stat_lane = iota((16, STAT), 1) < STAT // 2

    def attend(p):
        for i in (0, 1):
            b = 2 * p + i
            s = sbuf[p % 2, i] * scale
            pos = me * shard + iota(s.shape, 1)
            s = jnp.where(pos < len_s[b], s, -jnp.inf)
            m = jnp.max(s, axis=1, keepdims=True)
            e = jnp.exp(s - jnp.where(m > -jnp.inf, m, 0.0))
            l = jnp.sum(e, axis=1, keepdims=True)
            acc = dot(e.astype(BF16), ckv_v[b])
            stat = jnp.where(stat_lane, m, l)
            for k in (0, 1):
                acc_src[k, b, :, 0:lat] = acc[8 * k:8 * k + 8]
                acc_src[k, b, :, lat:lat + STAT] = stat[8 * k:8 * k + 8]

    groups = ((0, 4), (4, 8), (8, 12), (12, 14), (14, n_pair))
    n_full = 3
    sends = ((0, 1), (2, 3), (4, 5), (6, 7), (8, 9), (10, 11), (12,), (13,), (14,), (15,))

    def pair_copy(ps):
        rows = slice(2 * ps[0], 2 * ps[-1] + 2)
        return remote(acc_src.at[1 - c, rows], r1.at[rows], sent, a_recv.at[sends.index(ps)], sib)

    def chip_copy(ps):
        rows = slice(ps[0], ps[-1] + 1)
        g = max(i for i, group in enumerate(groups) if group[0] <= ps[0])
        return remote(s2.at[rows], r2.at[rows], sent, c_recv.at[g], cnt)

    def chip_wait(g):
        rows = r2.at[groups[g][0]:groups[g][1]]
        remote(rows, rows, sent, c_recv.at[g], cnt).wait_recv()

    def merge(a, b):
        m1, l1 = a[:, lat:lat + 1], a[:, lat + STAT // 2:lat + STAT // 2 + 1]
        m2, l2 = b[:, lat:lat + 1], b[:, lat + STAT // 2:lat + STAT // 2 + 1]
        m = jnp.maximum(m1, m2)
        shift = jnp.where(m > -jnp.inf, m, 0.0)
        w1, w2 = jnp.exp(m1 - shift), jnp.exp(m2 - shift)
        return w1 * a[:, :lat] + w2 * b[:, :lat], m, w1 * l1 + w2 * l2

    stat_lane8 = iota((8, STAT), 1) < STAT // 2

    def merge_pair(p):
        both = []
        for i in (0, 1):
            acc, m, l = merge(acc_src[c, 2 * p + i], r1[2 * p + i])
            both.append((acc, jnp.where(stat_lane8, m, l)))
        for k, (lo, hi) in enumerate(((0, lat), (lat, lat + STAT))):
            upper = upper8[:, lo:hi]
            zero = jnp.where(upper, both[0][k], both[1][k])
            one = jnp.where(upper, both[1][k], both[0][k])
            keep_v[p, :, lo:hi] = jnp.where(x == 0, zero, one)
            s2[p, :, lo:hi] = jnp.where(x == 0, one, zero)

    def o_rows(p):
        acc, _, l = merge(keep_v[p], r2[p])
        return acc / l

    def project(first, last):
        n_out, n_b = 8 * (last - first), 2 * (last - first)
        o_lat = jnp.concatenate([o_rows(p) for p in range(first, last)], axis=0).astype(BF16)
        head = iota((n_out, nope), 0) % 4
        wide = []
        for h in range(0, n_head, 2):
            two = dot(o_lat, jnp.concatenate([wuv_v[h], wuv_v[h + 1]], axis=1))
            wide += [jnp.where(head == h + i, two[:, i * nope:(i + 1) * nope], 0.0).astype(BF16) for i in (0, 1)]
        wide = jnp.concatenate(wide, axis=1)
        r = iota((n_b, n_out), 1)
        gather = (iota((n_b, n_out), 0) == row_of(r)).astype(F32).astype(BF16)
        o_val = dot(gather, wide).astype(BF16)
        return lambda k: dot(o_val, wo_v[:, pl.ds(pl.multiple_of(k * half_d, half_d), half_d)])

    def project_full(g):
        y = project(*groups[g])
        for k in (0, 1):
            y_src[g, k] = y(k)

    def project_last(g):
        y = project(*groups[g])
        i = g - n_full
        l_src[i, 1 - c] = y(1 - c)
        remote(l_src.at[i, 1 - c], l_r1.at[i], sent, a_recv.at[i], sib).start()
        l_src[i, c] = y(c)

    def y_copy(kind, g):
        if kind == 0:
            return remote(y_src.at[g, 1 - c], yr1.at[g], sent, q_recv.at[g], sib)
        return remote(yc.at[g], yr2.at[g], sent, q_recv.at[(3, 5, 6)[g]], cnt)

    def f_copy(g):
        return remote(f_src.at[g], f_rcv.at[g], sent, a_recv.at[2], sib)

    def last_chip(g):
        i = g - n_full
        remote(l_r1.at[i], l_r1.at[i], sent, a_recv.at[i], sib).wait_recv()
        l_sum[i] = l_src[i, c] + l_r1[i]
        for k, peer in enumerate((cnt, far, sib)[:1 + 2 * i]):
            remote(l_sum.at[i], l_all.at[i, k], sent, (q_recv.at[4], c_recv.at[0])[i], peer).start()

    def rows_of(g):
        return slice(2 * groups[g][0] % 8, (2 * groups[g][1] - 1) % 8 + 1)

    def half_copy():
        return remote(h_src, h_rcv, sent, a_recv.at[3], sib)

    def half_final(g):
        i = g - n_full
        remote(l_all.at[i, 0], l_all.at[i, 0], sent, (q_recv.at[4], c_recv.at[0])[i], sib).wait_recv()
        h_src[...] = (hid_half(2 * groups[g][0] // 8, c, rows_of(g)) + (l_sum[i] + l_all[i, 0])).astype(BF16)
        half_copy().start()

    def last_final(g):
        i = g - n_full
        remote(l_all.at[i], l_all.at[i], sent, (q_recv.at[4], c_recv.at[0])[i], sib).wait_recv()
        put(2 * groups[g][0] // 8, rows_of(g), l_sum[i] + l_all[i, 0], l_all[i, 2] + l_all[i, 1])

    def join(g, rows, mine, other):
        mine, other = mine.astype(F32), other.astype(F32)
        out_ref[g, rows, 0:half_d] = jnp.where(c == 0, mine, other).astype(BF16)
        out_ref[g, rows, half_d:d_model] = jnp.where(c == 0, other, mine).astype(BF16)

    def y_chip(g):
        y_copy(0, g).wait_recv()
        yc[g] = y_src[g, c] + yr1[g]
        y_copy(1, g).start()

    def hid_half(g, k, rows=slice(None)):
        return hid3_v[g, rows, pl.ds(pl.multiple_of(k * half_d, half_d), half_d)].astype(F32)

    def y_final(g):
        y_copy(1, g).wait_recv()
        f_src[g] = (hid_half(g, c) + (yc[g] + yr2[g])).astype(BF16)
        f_copy(g).start()

    def put(g, rows, mine, other):
        hid = hid3_v[g, rows, :].astype(F32)
        out_ref[g, rows, 0:half_d] = (hid[:, :half_d] + jnp.where(c == 0, mine, other)).astype(BF16)
        out_ref[g, rows, half_d:d_model] = (hid[:, half_d:] + jnp.where(c == 0, other, mine)).astype(BF16)

    def step(js, merges=(), ready=()):
        for j in js:
            wait_rows(j)
        if merges:
            pair_copy(merges).wait_recv()
        for g in ready:
            chip_wait(g)
        for j in js:
            scores(j)
            attend(j - 1)
        for p in merges:
            merge_pair(p)
        for g in ready:
            project_full(g)
        pair_copy(tuple(j - 1 for j in js)).start()
        if merges:
            chip_copy(merges).start()
        for g in ready:
            y_copy(0, g).start()

    q_wait(0)
    for g in range(n_direct, len(chunks)):
        for kind in (0, 2):
            q_copy(kind, g).start()
    wait_rows(0)
    scores(0)
    q_wait(1)
    step((1, 2))
    q_wait(2)
    step((3, 4))
    q_forward(3)
    step((5, 6), (0, 1))
    q_forward(4)
    q_wait(3)
    step((7, 8), (2, 3))
    step((9, 10), (4, 5))
    q_wait(4)
    step((11, 12), (6, 7))
    for w in late:
        w.wait()
    step((13,), (8, 9), (0,))
    step((14,), (10, 11))
    step((15,), (12,))
    attend(n_pair - 1)
    pair_copy((n_pair - 1,)).start()

    def last_merge(ps):
        pair_copy(ps).wait_recv()
        for p in ps:
            merge_pair(p)
        chip_copy(ps).start()

    last_merge((13,))
    last_merge((14,))
    last_merge((15,))
    for g in (1, 2):
        chip_wait(g)
        project_full(g)
        y_copy(0, g).start()
    y_chip(0)
    y_chip(1)
    chip_wait(3)
    project_last(3)
    y_chip(2)
    chip_wait(4)
    project_last(4)
    last_chip(3)
    last_chip(4)
    for g in range(n_full):
        y_final(g)
    half_final(3)
    remote(f_rcv, f_rcv, sent, a_recv.at[2], sib).wait_recv()
    for g in range(n_full):
        join(g, slice(None), f_src[g], f_rcv[g])
    half_copy().wait_recv()
    join(2 * groups[3][0] // 8, rows_of(3), h_src[...], h_rcv[...])
    half_copy().wait_send()
    remote(qall.at[0:3], qall.at[0:3], sent, q_recv.at[0], sib).wait_send()
    remote(r1, r1, sent, a_recv.at[0], sib).wait_send()
    remote(r2, r2, sent, c_recv.at[0], cnt).wait_send()
    remote(f_rcv, f_rcv, sent, a_recv.at[2], sib).wait_send()
    remote(y_src, y_src, sent, q_recv.at[0], sib).wait_send()
    remote(l_r1, l_r1, sent, a_recv.at[0], sib).wait_send()
    remote(l_src, l_src, sent, a_recv.at[0], sib).wait_send()
    last_final(4)


def solution(mesh):
    row_spec = P('batch', None)
    cache_spec = P('batch', 'seq', None)
    in_specs = (row_spec, P('batch'), cache_spec, cache_spec, P(None, 'seq', None), P(None, 'seq', None), P('seq', None, None), P('seq', None, None), P('seq', None, None))

    def mla_step(hidden, lengths, c_kv, k_rope, w_uq, w_qr, w_uk, w_uv, w_o):
        n_rows, d_model = hidden.shape
        _, shard, lat = c_kv.shape
        rope = k_rope.shape[2]
        n_head, nope = w_uq.shape[1], w_uq.shape[2]
        n_pair = n_rows // 2
        n_group = n_pair // GROUP
        wide = lat + STAT
        half = d_model // 2
        hid3 = hidden.reshape(n_group, 8, d_model)
        operands = (
            lengths,
            hidden,
            hid3,
            w_uq.reshape(d_model * n_head, nope),
            jnp.transpose(w_qr, (1, 2, 0)).reshape(n_head * rope, d_model),
            w_uk.reshape(n_head * nope, lat),
            w_uv,
            w_o.reshape(n_head * w_o.shape[1], d_model),
            c_kv,
            jnp.transpose(k_rope, (0, 2, 1)),
        )
        operands = tuple(pltpu.with_memory_space_constraint(a, pltpu.HBM) for a in operands)
        vm = pltpu.VMEM
        dma = pltpu.SemaphoreType.DMA
        out = pl.pallas_call(
            kernel,
            out_shape=jax.ShapeDtypeStruct((n_group, 8, d_model), BF16),
            in_specs=[pl.BlockSpec(memory_space=pltpu.HBM)] * len(operands),
            out_specs=pl.BlockSpec(memory_space=pltpu.VMEM),
            scratch_shapes=[
                pltpu.SMEM((n_rows,), jnp.int32),
                vm(hidden.shape, BF16),
                vm(hid3.shape, BF16),
                vm((n_head * n_rows, d_model), BF16),
                vm(operands[3].shape, BF16),
                vm(operands[4].shape, BF16),
                vm(operands[5].shape, BF16),
                vm(operands[6].shape, BF16),
                vm(operands[7].shape, BF16),
                vm(c_kv.shape, BF16),
                vm(operands[9].shape, BF16),
                vm((n_head * n_rows, n_head * d_model), BF16),
                vm((4, n_pair, 8, wide), BF16),
                vm((2, 2, 16, shard), F32),
                vm((2, n_rows, 8, wide), F32),
                vm((n_rows, 8, wide), F32),
                vm((n_pair, 8, wide), F32),
                vm((n_pair, 8, wide), F32),
                vm((n_pair, 8, wide), F32),
                vm((3, 2, 8, half), F32),
                vm((3, 8, half), F32),
                vm((3, 8, half), F32),
                vm((3, 8, half), F32),
                vm((3, 8, half), BF16),
                vm((3, 8, half), BF16),
                vm((4, half), BF16),
                vm((4, half), BF16),
                vm((2, 2, 4, half), F32),
                vm((2, 4, half), F32),
                vm((2, 4, half), F32),
                vm((2, 3, 4, half), F32),
                dma((5,)),
                dma((5,)),
                dma(()),
                dma((7,)),
                dma((10,)),
                dma((5,)),
            ],
            compiler_params=pltpu.CompilerParams(
                collective_id=0, has_side_effects=True, vmem_limit_bytes=53 * 1024 * 1024,
            ),
            name="mla_decode",
        )(*operands)
        return out.reshape(n_rows, d_model)

    return jax.shard_map(mla_step, mesh=mesh, in_specs=in_specs, out_specs=row_spec, check_vma=False)
```

```python
import math

import jax
import jax.numpy as jnp
from jax import lax
from jax.experimental import pallas as pl
from jax.experimental.pallas import tpu as pltpu
from jax.sharding import PartitionSpec as P

MESH = pl.DeviceIdType.MESH
F32 = jnp.float32
BF16 = jnp.bfloat16
GROUP = 4
STAT = 128


def dot(a, b):
    return jnp.dot(a, b, preferred_element_type=F32)


def dot_t(a, b):
    return lax.dot_general(a, b, (((1,), (1,)), ((), ())), preferred_element_type=F32)


def iota(shape, dim):
    return lax.broadcasted_iota(jnp.int32, shape, dim)


def kernel(
    len_hbm, hid_hbm, hid3_hbm, wuq_hbm, wqr_hbm, wuk_hbm, wuv_hbm, wo_hbm, ckv_hbm, kr_hbm,
    out_ref,
    len_s, hid_v, hid3_v, hid_r, wuq_v, wqr_v, wuk_v, wuv_v, wo_v, ckv_v, kr_v,
    em_v, qall, sbuf, acc_src, r1, s2, keep_v, r2, y_src, yr1, yc, yr2, f_src, f_rcv, h_src, h_rcv, l_src, l_r1, l_sum, l_all,
    w_sem, ckv_sem, sent, q_recv, a_recv, c_recv,
):
    n_rows = ckv_hbm.shape[0]
    shard = ckv_hbm.shape[1]
    lat = ckv_hbm.shape[2]
    rope = kr_hbm.shape[1]
    nope = wuq_hbm.shape[1]
    n_pair = n_rows // 2
    d_model = hid_hbm.shape[1]
    half_d = d_model // 2
    scale = 1.0 / math.sqrt(nope + rope)

    me = lax.axis_index("seq")
    x = lax.div(me, 2)
    c = lax.rem(me, 2)
    sib = 2 * x + (1 - c)
    cnt = 2 * (1 - x) + c
    far = 3 - me

    def load(src, dst, sem):
        return pltpu.make_async_copy(src, dst, sem)

    hid_load = load(hid_hbm, hid_v, w_sem.at[0])
    early = [load(src, dst, w_sem.at[min(1 + i, 3)]) for i, (src, dst) in enumerate((
        (wqr_hbm, wqr_v), (wuq_hbm, wuq_v), (wuk_hbm, wuk_v), (len_hbm, len_s), (hid3_hbm, hid3_v)))]
    late = [load(src, dst, w_sem.at[4]) for src, dst in ((wuv_hbm, wuv_v), (wo_hbm, wo_v))]
    spans = ((0, 1), (1, 3), (3, 7), (7, 11), (11, n_pair))

    def row_loads(i):
        rows = slice(2 * spans[i][0], 2 * spans[i][1])
        return (load(kr_hbm.at[rows], kr_v.at[rows], ckv_sem.at[i]), load(ckv_hbm.at[rows], ckv_v.at[rows], ckv_sem.at[i]))

    for w in (hid_load, *early):
        w.start()

    barrier = pltpu.get_barrier_semaphore()
    for peer in (sib, cnt, far):
        pl.semaphore_signal(barrier, inc=1, device_id={"seq": peer}, device_id_type=MESH)

    for i in range(len(spans)):
        for w in row_loads(i):
            w.start()
        if i == 2:
            for w in late:
                w.start()

    def remote(src, dst, send, recv, peer):
        return pltpu.make_async_remote_copy(
            src_ref=src, dst_ref=dst, send_sem=send, recv_sem=recv,
            device_id={"seq": peer}, device_id_type=MESH,
        )

    n_head = wqr_hbm.shape[0] // rope
    n_local = n_rows * n_head
    def row_of(r):
        j = (r // 4) % 2
        return 2 * (r // 8) + j + x - 2 * j * x

    r_h = iota((n_local, nope), 0) % 4
    same_head = iota((n_local, n_head * nope), 1) % n_head == iota((n_local, n_head * nope), 0) % 4
    spread = (iota((nope, n_head * nope), 1) // n_head == iota((nope, n_head * nope), 0)).astype(F32).astype(BF16)
    rep = (iota((n_local, n_rows), 1) == row_of(iota((n_local, n_rows), 0))).astype(F32).astype(BF16)
    fold = (iota((n_head * rope, STAT), 0) % rope == iota((n_head * rope, STAT), 1)).astype(F32).astype(BF16)
    hid_load.wait()
    hid_r[...] = dot(rep, hid_v[...]).astype(BF16)
    for k in range(d_model // nope):
        wide = dot(hid_r[:, k * nope:(k + 1) * nope], spread)
        em_v[:, k * n_head * nope:(k + 1) * n_head * nope] = jnp.where(same_head, wide, 0.0).astype(BF16)
    for w in early[:2]:
        w.wait()
    q_r = dot_t(hid_r[...], wqr_v[...])
    q_n = dot(em_v[...], wuq_v[...])
    q_r = jnp.where(iota((n_local, n_head * rope), 1) // rope == iota((n_local, n_head * rope), 0) % 4, q_r, 0.0)
    q_r = dot(q_r.astype(BF16), fold).astype(BF16)
    q_wide = jnp.concatenate([jnp.where(r_h == h, q_n, 0.0).astype(BF16) for h in range(n_head)], axis=1)
    for w in early[2:]:
        w.wait()
    q_l = dot(q_wide, wuk_v[...]).astype(BF16)
    for p in range(n_pair):
        qall[me, p, :, 0:lat] = q_l[8 * p:8 * p + 8]
        qall[me, p, :, lat:lat + STAT] = q_r[8 * p:8 * p + 8]

    pl.semaphore_wait(barrier, 3)

    chunks = ((0, 1), (1, 3), (3, 7), (7, 11), (11, n_pair))
    n_direct = 3

    def q_copy(kind, g):
        forward = g >= n_direct and kind == 1
        first = cnt if g >= n_direct else 2 * (1 - x)
        slot, peer = ((me, first), (cnt, sib) if forward else (me, 2 * (1 - x) + 1), (me, sib))[kind]
        rows = qall.at[slot, chunks[g][0]:chunks[g][1]]
        return remote(rows, rows, sent, q_recv.at[g + 2 if g >= n_direct and kind == 0 else g], peer)

    def q_wait(g):
        rows = qall.at[0:2 if g >= n_direct else 3, chunks[g][0]:chunks[g][1]]
        remote(rows, rows, sent, q_recv.at[g], sib).wait_recv()

    def q_forward(g):
        q_copy(0, g).wait_recv()
        q_copy(1, g).start()

    for g in range(n_direct):
        for kind in range(3):
            q_copy(kind, g).start()


    upper8 = iota((8, lat + STAT), 0) < 4

    def scores(p):
        tiles = [qall[s, p].astype(F32) for s in range(4)]
        q_even = jnp.concatenate([jnp.where(upper8, tiles[0], tiles[2]), jnp.where(upper8, tiles[1], tiles[3])], axis=0)
        q_odd = jnp.concatenate([jnp.where(upper8, tiles[2], tiles[0]), jnp.where(upper8, tiles[3], tiles[1])], axis=0)
        for i, q in enumerate((q_even, q_odd)):
            q = q.astype(BF16)
            b = 2 * p + i
            s = dot_t(q[:, :lat], ckv_v[b]) + dot(q[:, lat:lat + rope], kr_v[b])
            sbuf[p % 2, i] = s

    def wait_rows(p):
        for i, span in enumerate(spans):
            if p == span[0]:
                for w in row_loads(i):
                    w.wait()

    stat_lane = iota((16, STAT), 1) < STAT // 2

    def attend(p):
        for i in (0, 1):
            b = 2 * p + i
            s = sbuf[p % 2, i] * scale
            pos = me * shard + iota(s.shape, 1)
            s = jnp.where(pos < len_s[b], s, -jnp.inf)
            m = jnp.max(s, axis=1, keepdims=True)
            e = jnp.exp(s - jnp.where(m > -jnp.inf, m, 0.0))
            l = jnp.sum(e, axis=1, keepdims=True)
            acc = dot(e.astype(BF16), ckv_v[b])
            stat = jnp.where(stat_lane, m, l)
            for k in (0, 1):
                acc_src[k, b, :, 0:lat] = acc[8 * k:8 * k + 8]
                acc_src[k, b, :, lat:lat + STAT] = stat[8 * k:8 * k + 8]

    groups = ((0, 4), (4, 8), (8, 12), (12, 14), (14, n_pair))
    n_full = 3
    sends = ((0, 1), (2, 3), (4, 5), (6, 7), (8, 9), (10, 11), (12,), (13,), (14,), (15,))

    def pair_copy(ps):
        rows = slice(2 * ps[0], 2 * ps[-1] + 2)
        i = sends.index(ps)
        return remote(acc_src.at[1 - c, rows], r1.at[rows], sent, a_recv.at[i] if i < 6 else ckv_sem.at[i - 6], sib)

    def chip_copy(ps):
        rows = slice(ps[0], ps[-1] + 1)
        g = max(i for i, group in enumerate(groups) if group[0] <= ps[0])
        return remote(s2.at[rows], r2.at[rows], sent, c_recv.at[g], cnt)

    def chip_wait(g):
        rows = r2.at[groups[g][0]:groups[g][1]]
        remote(rows, rows, sent, c_recv.at[g], cnt).wait_recv()

    def merge(a, b):
        m1, l1 = a[:, lat:lat + 1], a[:, lat + STAT // 2:lat + STAT // 2 + 1]
        m2, l2 = b[:, lat:lat + 1], b[:, lat + STAT // 2:lat + STAT // 2 + 1]
        m = jnp.maximum(m1, m2)
        shift = jnp.where(m > -jnp.inf, m, 0.0)
        w1, w2 = jnp.exp(m1 - shift), jnp.exp(m2 - shift)
        return w1 * a[:, :lat] + w2 * b[:, :lat], m, w1 * l1 + w2 * l2

    stat_lane8 = iota((8, STAT), 1) < STAT // 2

    def merge_pair(p):
        both = []
        for i in (0, 1):
            acc, m, l = merge(acc_src[c, 2 * p + i], r1[2 * p + i])
            both.append((acc, jnp.where(stat_lane8, m, l)))
        for k, (lo, hi) in enumerate(((0, lat), (lat, lat + STAT))):
            upper = upper8[:, lo:hi]
            zero = jnp.where(upper, both[0][k], both[1][k])
            one = jnp.where(upper, both[1][k], both[0][k])
            keep_v[p, :, lo:hi] = jnp.where(x == 0, zero, one)
            s2[p, :, lo:hi] = jnp.where(x == 0, one, zero)

    def o_rows(p):
        acc, _, l = merge(keep_v[p], r2[p])
        return acc / l

    def project(first, last):
        n_out, n_b = 8 * (last - first), 2 * (last - first)
        o_lat = jnp.concatenate([o_rows(p) for p in range(first, last)], axis=0).astype(BF16)
        head = iota((n_out, nope), 0) % 4
        wide = []
        for h in range(0, n_head, 2):
            two = dot(o_lat, jnp.concatenate([wuv_v[h], wuv_v[h + 1]], axis=1))
            wide += [jnp.where(head == h + i, two[:, i * nope:(i + 1) * nope], 0.0).astype(BF16) for i in (0, 1)]
        wide = jnp.concatenate(wide, axis=1)
        r = iota((n_b, n_out), 1)
        gather = (iota((n_b, n_out), 0) == row_of(r)).astype(F32).astype(BF16)
        o_val = dot(gather, wide).astype(BF16)
        return lambda k: dot(o_val, wo_v[:, pl.ds(pl.multiple_of(k * half_d, half_d), half_d)])

    def project_full(g):
        y = project(*groups[g])
        for k in (0, 1):
            y_src[g, k] = y(k)

    def project_last(g):
        y = project(*groups[g])
        i = g - n_full
        l_src[i, 1 - c] = y(1 - c)
        remote(l_src.at[i, 1 - c], l_r1.at[i], sent, a_recv.at[i], sib).start()
        l_src[i, c] = y(c)

    def y_copy(kind, g):
        if kind == 0:
            return remote(y_src.at[g, 1 - c], yr1.at[g], sent, q_recv.at[g], sib)
        return remote(yc.at[g], yr2.at[g], sent, q_recv.at[(3, 5, 6)[g]], cnt)

    def f_copy(g):
        return remote(f_src.at[g], f_rcv.at[g], sent, a_recv.at[2], sib)

    def last_chip(g):
        i = g - n_full
        remote(l_r1.at[i], l_r1.at[i], sent, a_recv.at[i], sib).wait_recv()
        l_sum[i] = l_src[i, c] + l_r1[i]
        for k, peer in enumerate((cnt, far, sib)[:1 + 2 * i]):
            remote(l_sum.at[i], l_all.at[i, k], sent, (q_recv.at[4], c_recv.at[0])[i], peer).start()

    def rows_of(g):
        return slice(2 * groups[g][0] % 8, (2 * groups[g][1] - 1) % 8 + 1)

    def half_copy():
        return remote(h_src, h_rcv, sent, a_recv.at[3], sib)

    def half_final(g):
        i = g - n_full
        remote(l_all.at[i, 0], l_all.at[i, 0], sent, (q_recv.at[4], c_recv.at[0])[i], sib).wait_recv()
        h_src[...] = (hid_half(2 * groups[g][0] // 8, c, rows_of(g)) + (l_sum[i] + l_all[i, 0])).astype(BF16)
        half_copy().start()

    def last_final(g):
        i = g - n_full
        remote(l_all.at[i], l_all.at[i], sent, (q_recv.at[4], c_recv.at[0])[i], sib).wait_recv()
        put(2 * groups[g][0] // 8, rows_of(g), l_sum[i] + l_all[i, 0], l_all[i, 2] + l_all[i, 1])

    def join(g, rows, mine, other):
        mine, other = mine.astype(F32), other.astype(F32)
        out_ref[g, rows, 0:half_d] = jnp.where(c == 0, mine, other).astype(BF16)
        out_ref[g, rows, half_d:d_model] = jnp.where(c == 0, other, mine).astype(BF16)

    def y_chip(g):
        y_copy(0, g).wait_recv()
        yc[g] = y_src[g, c] + yr1[g]
        y_copy(1, g).start()

    def hid_half(g, k, rows=slice(None)):
        return hid3_v[g, rows, pl.ds(pl.multiple_of(k * half_d, half_d), half_d)].astype(F32)

    def y_final(g):
        y_copy(1, g).wait_recv()
        f_src[g] = (hid_half(g, c) + (yc[g] + yr2[g])).astype(BF16)
        f_copy(g).start()

    def put(g, rows, mine, other):
        hid = hid3_v[g, rows, :].astype(F32)
        out_ref[g, rows, 0:half_d] = (hid[:, :half_d] + jnp.where(c == 0, mine, other)).astype(BF16)
        out_ref[g, rows, half_d:d_model] = (hid[:, half_d:] + jnp.where(c == 0, other, mine)).astype(BF16)

    def step(js, merges=(), ready=()):
        for j in js:
            wait_rows(j)
        if merges:
            pair_copy(merges).wait_recv()
        for g in ready:
            chip_wait(g)
        for j in js:
            scores(j)
            attend(j - 1)
        for p in merges:
            merge_pair(p)
        for g in ready:
            project_full(g)
        pair_copy(tuple(j - 1 for j in js)).start()
        if merges:
            chip_copy(merges).start()
        for g in ready:
            y_copy(0, g).start()

    q_wait(0)
    for g in range(n_direct, len(chunks)):
        for kind in (0, 2):
            q_copy(kind, g).start()
    wait_rows(0)
    scores(0)
    q_wait(1)
    step((1, 2))
    q_wait(2)
    step((3, 4))
    q_forward(3)
    step((5, 6), (0, 1))
    q_forward(4)
    q_wait(3)
    step((7, 8), (2, 3))
    step((9, 10), (4, 5))
    q_wait(4)
    step((11, 12), (6, 7))
    for w in late:
        w.wait()
    step((13,), (8, 9), (0,))
    step((14,), (10, 11))
    step((15,), (12,))
    attend(n_pair - 1)
    pair_copy((n_pair - 1,)).start()

    def last_merge(ps):
        pair_copy(ps).wait_recv()
        for p in ps:
            merge_pair(p)
        chip_copy(ps).start()

    last_merge((13,))
    last_merge((14,))
    last_merge((15,))
    for g in (1, 2):
        chip_wait(g)
        project_full(g)
        y_copy(0, g).start()
    y_chip(0)
    y_chip(1)
    chip_wait(3)
    project_last(3)
    y_chip(2)
    chip_wait(4)
    project_last(4)
    last_chip(3)
    last_chip(4)
    for g in range(n_full):
        y_final(g)
    half_final(3)
    remote(f_rcv, f_rcv, sent, a_recv.at[2], sib).wait_recv()
    for g in range(n_full):
        join(g, slice(None), f_src[g], f_rcv[g])
    half_copy().wait_recv()
    join(2 * groups[3][0] // 8, rows_of(3), h_src[...], h_rcv[...])
    half_copy().wait_send()
    remote(qall.at[0:3], qall.at[0:3], sent, q_recv.at[0], sib).wait_send()
    remote(r1, r1, sent, a_recv.at[0], sib).wait_send()
    remote(r2, r2, sent, c_recv.at[0], cnt).wait_send()
    remote(f_rcv, f_rcv, sent, a_recv.at[2], sib).wait_send()
    remote(y_src, y_src, sent, q_recv.at[0], sib).wait_send()
    remote(l_r1, l_r1, sent, a_recv.at[0], sib).wait_send()
    remote(l_src, l_src, sent, a_recv.at[0], sib).wait_send()
    last_final(4)


def solution(mesh):
    row_spec = P('batch', None)
    cache_spec = P('batch', 'seq', None)
    in_specs = (row_spec, P('batch'), cache_spec, cache_spec, P(None, 'seq', None), P(None, 'seq', None), P('seq', None, None), P('seq', None, None), P('seq', None, None))

    def mla_step(hidden, lengths, c_kv, k_rope, w_uq, w_qr, w_uk, w_uv, w_o):
        n_rows, d_model = hidden.shape
        _, shard, lat = c_kv.shape
        rope = k_rope.shape[2]
        n_head, nope = w_uq.shape[1], w_uq.shape[2]
        n_pair = n_rows // 2
        n_group = n_pair // GROUP
        wide = lat + STAT
        half = d_model // 2
        hid3 = hidden.reshape(n_group, 8, d_model)
        operands = (
            lengths,
            hidden,
            hid3,
            w_uq.reshape(d_model * n_head, nope),
            jnp.transpose(w_qr, (1, 2, 0)).reshape(n_head * rope, d_model),
            w_uk.reshape(n_head * nope, lat),
            w_uv,
            w_o.reshape(n_head * w_o.shape[1], d_model),
            c_kv,
            jnp.transpose(k_rope, (0, 2, 1)),
        )
        operands = tuple(pltpu.with_memory_space_constraint(a, pltpu.HBM) for a in operands)
        vm = pltpu.VMEM
        dma = pltpu.SemaphoreType.DMA
        out = pl.pallas_call(
            kernel,
            out_shape=jax.ShapeDtypeStruct((n_group, 8, d_model), BF16),
            in_specs=[pl.BlockSpec(memory_space=pltpu.HBM)] * len(operands),
            out_specs=pl.BlockSpec(memory_space=pltpu.VMEM),
            scratch_shapes=[
                pltpu.SMEM((n_rows,), jnp.int32),
                vm(hidden.shape, BF16),
                vm(hid3.shape, BF16),
                vm((n_head * n_rows, d_model), BF16),
                vm(operands[3].shape, BF16),
                vm(operands[4].shape, BF16),
                vm(operands[5].shape, BF16),
                vm(operands[6].shape, BF16),
                vm(operands[7].shape, BF16),
                vm(c_kv.shape, BF16),
                vm(operands[9].shape, BF16),
                vm((n_head * n_rows, n_head * d_model), BF16),
                vm((4, n_pair, 8, wide), BF16),
                vm((2, 2, 16, shard), F32),
                vm((2, n_rows, 8, wide), F32),
                vm((n_rows, 8, wide), F32),
                vm((n_pair, 8, wide), F32),
                vm((n_pair, 8, wide), F32),
                vm((n_pair, 8, wide), F32),
                vm((3, 2, 8, half), F32),
                vm((3, 8, half), F32),
                vm((3, 8, half), F32),
                vm((3, 8, half), F32),
                vm((3, 8, half), BF16),
                vm((3, 8, half), BF16),
                vm((4, half), BF16),
                vm((4, half), BF16),
                vm((2, 2, 4, half), F32),
                vm((2, 4, half), F32),
                vm((2, 4, half), F32),
                vm((2, 3, 4, half), F32),
                dma((5,)),
                dma((5,)),
                dma(()),
                dma((7,)),
                dma((6,)),
                dma((5,)),
            ],
            compiler_params=pltpu.CompilerParams(
                collective_id=0, has_side_effects=True, vmem_limit_bytes=53 * 1024 * 1024,
            ),
            name="mla_decode",
        )(*operands)
        return out.reshape(n_rows, d_model)

    return jax.shard_map(mla_step, mesh=mesh, in_specs=in_specs, out_specs=row_spec, check_vma=False)
```
